32 devices in a mesh: rep: 1 (over z), dp: 32 (over x, y, core).
Axes of the slice: x: 4, y: 4, z: 1, core: 2. Of those that a mesh axis runs over, the one named last changes fastest.
The devices are a block of a 4x4x8 slice.
Arguments:
- x: bfloat16 [32, 2048, 512], P(('rep', 'dp'))
- dy: bfloat16 [32, 2048, 512], P(('rep', 'dp'))
- w_gate: bfloat16 [2, 512, 3072], P(None, 'dp')
- w_up: bfloat16 [2, 512, 3072], P(None, 'dp')
- w_down: bfloat16 [2, 3072, 512], P(None, 'dp')
- m_w_gate: float32 [2, 512, 3072], P(None, 'dp')
- m_w_up: float32 [2, 512, 3072], P(None, 'dp')
- m_w_down: float32 [2, 3072, 512], P(None, 'dp')
- v_w_gate: float32 [2, 512, 3072], P(None, 'dp')
- v_w_up: float32 [2, 512, 3072], P(None, 'dp')
- v_w_down: float32 [2, 3072, 512], P(None, 'dp')
Outputs:
- output 1: bfloat16 [2, 512, 3072], P('rep', 'dp')
- output 2: bfloat16 [2, 512, 3072], P('rep', 'dp')
- output 3: bfloat16 [2, 3072, 512], P('rep', 'dp')
- output 4: float32 [2, 512, 3072], P('rep', 'dp')
- output 5: float32 [2, 512, 3072], P('rep', 'dp')
- output 6: float32 [2, 3072, 512], P('rep', 'dp')
- output 7: float32 [2, 512, 3072], P('rep', 'dp')
- output 8: float32 [2, 512, 3072], P('rep', 'dp')
- output 9: float32 [2, 3072, 512], P('rep', 'dp')
All inputs are finite; a program needn't handle non-finite values.
Results may differ from the reference program's by a relative error of at most 0.022.
Values are sent between devices in bfloat16 or wider.
A program may use at most 768 MiB of HBM per device.

```python
import jax
import jax.numpy as jnp
from jax import lax

SEQUENCES = 32
TOKENS = 2048
D = 512
FF = 3072
LAYERS = 2
NAMES = ("w_gate", "w_up", "w_down")
SHAPES = {"w_gate": (LAYERS, D, FF), "w_up": (LAYERS, D, FF), "w_down": (LAYERS, FF, D)}


def bump(key, n, height):
    away = (jnp.arange(n, dtype=jnp.int32) - jax.random.randint(key, (), 0, n, jnp.int32)) % n
    return jnp.where(away < n // 8, height, 1.0)


def together(key, own, strength):
    shared = jax.random.normal(key, own.shape[1:], jnp.float32)
    return (own + strength * shared) * lax.rsqrt(1 + strength * strength)


def setup_inputs(seed: int = 0, part: int = 0) -> dict:
    kx, kdy, ka, kb, kz, kf, kh, kl, *keys = jax.random.split(jax.random.key(seed), 8 + 3 * len(NAMES))
    kx, kdy, ka, kb = (jax.random.fold_in(k, part) for k in (kx, kdy, ka, kb))
    kw, km, kv = (keys[i::3] for i in range(3))
    shape = (SEQUENCES, TOKENS, D)
    much_x, much_dy = jax.random.uniform(kz, (2,), jnp.float32, 0.0, 1.0)
    loud = 2.0 ** jax.random.uniform(jax.random.fold_in(kz, 1), (), jnp.float32, -1.0, 2.0)
    layers = 2.0 ** jax.random.uniform(kl, (LAYERS, 1, 1), jnp.float32, -1.0, 1.0)
    x = together(ka, jax.random.normal(kx, shape, jnp.float32), much_x) * bump(kf, D, 4.0)
    dy = together(kb, jax.random.normal(kdy, shape, jnp.float32), much_dy)
    drawn = {"x": x.astype(jnp.bfloat16), "dy": (loud * dy * (SEQUENCES * TOKENS) ** -0.5).astype(jnp.bfloat16)}
    for key, name in zip(kw, NAMES, strict=True):
        w = jax.random.normal(key, SHAPES[name], jnp.float32) * SHAPES[name][1] ** -0.5
        drawn[name] = (w * {"w_gate": 1.0, "w_up": bump(kh, FF, 4.0), "w_down": layers}[name]).astype(jnp.bfloat16)
    for key, name in zip(km, NAMES, strict=True):
        drawn[f"m_{name}"] = 0.1 * jax.random.normal(key, SHAPES[name], jnp.float32)
    for key, name in zip(kv, NAMES, strict=True):
        drawn[f"v_{name}"] = jax.random.uniform(key, SHAPES[name], jnp.float32, 0.005, 0.015)
    return drawn


def matmul(a, w):
    return jnp.dot(a, w, preferred_element_type=jnp.float32).astype(jnp.bfloat16)


def normed(h):
    wide = h.astype(jnp.float32)
    scale = lax.rsqrt(jnp.mean(wide**2, -1, keepdims=True) + 1e-6)
    return (wide * scale).astype(jnp.bfloat16)


def layer(h, w):
    a = normed(h)
    gate = jnp.dot(a, w["w_gate"], preferred_element_type=jnp.float32)
    up = jnp.dot(a, w["w_up"], preferred_element_type=jnp.float32)
    return h + matmul((jax.nn.silu(gate) * up).astype(jnp.bfloat16), w["w_down"])


def adamw(w, m, v, g):
    m = 0.9 * m + 0.1 * g
    v = 0.95 * v + 0.05 * g * g
    step = m * lax.rsqrt(v + 1e-8) + 0.1 * w
    return (w - 0.02 * step).astype(jnp.bfloat16), m, v


def clipped(gradients, sum_of_squares, count):
    factor = jnp.minimum(1.0, 0.5 * lax.rsqrt(sum_of_squares / count + 1e-30))
    return [g * factor for g in gradients]


def stack(weights, h):
    return lax.scan(lambda h, w: (layer(h, w), None), h, weights)[0]


def reference(x, dy, w_gate, w_up, w_down, m_w_gate, m_w_up, m_w_down, v_w_gate, v_w_up, v_w_down):
    weights = dict(zip(NAMES, (w_gate, w_up, w_down), strict=True))

    def take(so_far, sequence):
        h, by_y = sequence
        _, back = jax.vjp(lambda w: stack(w, h), weights)
        return jax.tree.map(lambda total, term: total + term.astype(jnp.float32), so_far, back(by_y)[0]), None

    none_yet = {name: jnp.zeros(w.shape, jnp.float32) for name, w in weights.items()}
    by_weights, _ = lax.scan(take, none_yet, (x, dy))
    gradients = [by_weights[name].astype(jnp.bfloat16).astype(jnp.float32) for name in NAMES]
    gradients = clipped(gradients, sum(jnp.sum(g * g) for g in gradients), sum(g.size for g in gradients))
    new = [
        adamw(w.astype(jnp.float32), m, v, g)
        for w, m, v, g in zip((w_gate, w_up, w_down), (m_w_gate, m_w_up, m_w_down), (v_w_gate, v_w_up, v_w_down), gradients, strict=True)
    ]
    return tuple(one[which] for which in range(3) for one in new)
```

```python
import functools
import math

import jax
import jax.numpy as jnp
from jax import lax
from jax.experimental import pallas as pl
from jax.experimental.pallas import tpu as pltpu
from jax.sharding import PartitionSpec as P

NAMES = ("w_gate", "w_up", "w_down")
MESH = pl.DeviceIdType.MESH
CORES = 2
VMEM = pl.BlockSpec(memory_space=pltpu.VMEM)
HBM = pl.BlockSpec(memory_space=pl.ANY)


def matmul(a, w):
    return jnp.dot(a, w, preferred_element_type=jnp.float32).astype(jnp.bfloat16)


def normed(h):
    wide = h.astype(jnp.float32)
    scale = lax.rsqrt(jnp.mean(wide**2, -1, keepdims=True) + 1e-6)
    return (wide * scale).astype(jnp.bfloat16)


def layer(h, w):
    a = normed(h)
    gate = jnp.dot(a, w["w_gate"], preferred_element_type=jnp.float32)
    up = jnp.dot(a, w["w_up"], preferred_element_type=jnp.float32)
    return h + matmul((jax.nn.silu(gate) * up).astype(jnp.bfloat16), w["w_down"])


def adamw(w, m, v, g):
    m = 0.9 * m + 0.1 * g
    v = 0.95 * v + 0.05 * g * g
    step = m * lax.rsqrt(v + 1e-8) + 0.1 * w
    return (w - 0.02 * step).astype(jnp.bfloat16), m, v


class Place:
    def __init__(self, side):
        self.side = side
        me = lax.axis_index("dp")
        self.c = lax.rem(me, CORES)
        self.y = lax.rem(me // CORES, side)
        self.x = me // (CORES * side)

    def device(self, x, y, c):
        return {"dp": (x * self.side + y) * CORES + c}

    def partner(self):
        return self.device(self.x, self.y, 1 - self.c)

    def along(self, axis, k):
        if axis == "x":
            x = lax.rem(self.x + k, self.side)
            return x, self.device(x, self.y, self.c)
        y = lax.rem(self.y + k, self.side)
        return y, self.device(self.x, y, self.c)

    def barrier(self):
        sem = pltpu.get_barrier_semaphore()
        others = [self.partner()] + [self.along(a, k)[1] for a in "xy" for k in range(1, self.side)]
        for other in others:
            pl.semaphore_signal(sem, inc=1, device_id=other, device_id_type=MESH)
        pl.semaphore_wait(sem, len(others))


def send(src, dst, sems, device):
    return pltpu.make_async_remote_copy(
        src_ref=src, dst_ref=dst, send_sem=sems[0], recv_sem=sems[1], device_id=device, device_id_type=MESH
    )


class Gather:
    def __init__(self, place, whole, send_sems, recv_sems, first):
        p, s = place, place.side
        sems = [(send_sems.at[i], recv_sems.at[i]) for i in range(2 * s - 1)]
        second = "y" if first == "x" else "x"
        own = whole.at[p.x, p.y, p.c]
        line = whole.at[:, p.y, p.c] if first == "x" else whole.at[p.x, :, p.c]
        plane = whole.at[:, :, p.c]
        self.stages = [
            [send(own, own, sems[k - 1], p.along(first, k)[1]) for k in range(1, s)],
            [send(line, line, sems[s - 2 + k], p.along(second, k)[1]) for k in range(1, s)],
            [send(plane, plane, sems[2 * s - 2], p.partner())],
        ]

    def start(self, stage):
        for copy in self.stages[stage]:
            copy.start()

    def wait(self, stage):
        for copy in self.stages[stage]:
            copy.wait()


def gather_kernel(side, *refs):
    shards, wholes, (send_sems, recv_sems, local_sems) = refs[:3], refs[3:9], refs[9:]
    p = Place(side)
    units = []
    for i, whole in enumerate(wholes):
        number, which = divmod(i, 3)
        pltpu.make_async_copy(shards[which].at[number], whole.at[p.x, p.y, p.c], local_sems.at[i]).start()
        units.append(Gather(p, whole, send_sems.at[i], recv_sems.at[i], "xy"[i % 2]))
    p.barrier()
    for i, whole in enumerate(wholes):
        number, which = divmod(i, 3)
        pltpu.make_async_copy(shards[which].at[number], whole.at[p.x, p.y, p.c], local_sems.at[i]).wait()
        units[i].start(0)
    for stage in range(3):
        for unit in units:
            unit.wait(stage)
            if stage < 2:
                unit.start(stage + 1)


def gathered(side, weights):
    layers = weights[0].shape[0]
    wholes = [jax.ShapeDtypeStruct((side, side, CORES) + w.shape[1:], w.dtype) for _ in range(layers) for w in weights]
    count = len(wholes)
    out = pl.pallas_call(
        functools.partial(gather_kernel, side),
        out_shape=wholes,
        in_specs=[HBM] * 3,
        out_specs=[HBM] * count,
        scratch_shapes=[
            pltpu.SemaphoreType.DMA((count, 2 * side - 1)),
            pltpu.SemaphoreType.DMA((count, 2 * side - 1)),
            pltpu.SemaphoreType.DMA((count,)),
        ],
        compiler_params=pltpu.CompilerParams(collective_id=0, has_side_effects=True),
        name="gather",
    )(*weights)
    return [w.reshape(-1, w.shape[-1]) for w in out]


class Scatter:
    def __init__(self, place, refs, send_sems, recv_sems, first):
        p, s = place, place.side
        self.p, self.s, self.first, self.refs = p, s, first, refs
        mine, pair, paired, line, lined, last, _ = refs
        sems = [(send_sems.at[i], recv_sems.at[i]) for i in range(2 * s - 1)]
        second = "y" if first == "x" else "x"
        self.stages = [[send(mine.at[:, :, 1 - p.c], pair, sems[0], p.partner())], [], []]
        for k in range(1, s):
            there, device = p.along(first, k)
            part = paired.at[there] if first == "x" else paired.at[:, there]
            self.stages[1].append(send(part, line.at[k - 1], sems[k], device))
        for k in range(1, s):
            there, device = p.along(second, k)
            self.stages[2].append(send(lined.at[there], last.at[k - 1], sems[s - 1 + k], device))

    def start(self, stage):
        for copy in self.stages[stage]:
            copy.start()

    def wait(self, stage):
        for copy in self.stages[stage]:
            copy.wait()

    def _pair_sum(self, x, y):
        mine, pair = self.refs[:2]
        return mine[x, y, self.p.c].astype(jnp.float32) + pair[x, y].astype(jnp.float32)

    def _line_sum(self, i):
        p, line = self.p, self.refs[3]
        total = self._pair_sum(p.x, i) if self.first == "x" else self._pair_sum(i, p.y)
        for k in range(self.s - 1):
            total += line[k, i].astype(jnp.float32)
        return total

    def add(self, stage):
        p, s = self.p, self.s
        mine, pair, paired, line, lined, last, out = self.refs
        if stage == 0:

            @pl.loop(0, s * s)
            def _(i):
                x, y = i // s, lax.rem(i, s)
                paired[x, y] = self._pair_sum(x, y).astype(paired.dtype)

        elif stage == 1:

            @pl.loop(0, s)
            def _(i):
                lined[i] = self._line_sum(i).astype(lined.dtype)

        else:
            total = self._line_sum(p.y if self.first == "x" else p.x)
            for k in range(s - 1):
                total += last[k].astype(jnp.float32)
            total = total.astype(out.dtype)
            out[...] = total
            return total


def scatter_kernel(side, count, *refs):
    grads, outs, norm = refs[:count], refs[count : 2 * count], refs[2 * count]
    rest = refs[2 * count + 1 :]
    tables = [rest[i * count : (i + 1) * count] for i in range(5)]
    squares, others, send_sems, recv_sems, norm_send, norm_recv = rest[5 * count :]
    p = Place(side)
    units = [
        Scatter(p, (grads[i], *(t[i] for t in tables), outs[i]), send_sems.at[i], recv_sems.at[i], "xy"[i % 2]) for i in range(count)
    ]
    p.barrier()
    for unit in units:
        unit.start(0)
    total = jnp.zeros((8, 128), jnp.float32)
    for stage in range(3):
        for unit in units:
            unit.wait(stage)
            g = unit.add(stage)
            if stage < 2:
                unit.start(stage + 1)
            else:
                wide = g.astype(jnp.float32)
                wide = wide * wide
                total += wide.reshape(-1, 8, 128).sum(0) if wide.shape[-1] == 128 else fold(wide)
    norm[...] = reduced(p, total, squares, others, norm_send, norm_recv)


def fold(wide):
    rows, columns = wide.shape
    rows8 = wide.reshape(rows // 8, 8, columns).sum(0)
    total = rows8[:, :128]
    for i in range(128, columns, 128):
        total += rows8[:, i : i + 128]
    return total


def reduced(p, total, squares, others, send_sems, recv_sems):
    at = 0
    for stage, devices in enumerate(
        ([p.partner()], [p.along("y", k)[1] for k in range(1, p.side)], [p.along("x", k)[1] for k in range(1, p.side)])
    ):
        squares[stage] = total
        copies = []
        for device in devices:
            copies.append(send(squares.at[stage], others.at[at], (send_sems.at[at], recv_sems.at[at]), device))
            at += 1
        for copy in copies:
            copy.start()
        for copy in copies:
            copy.wait()
        for i in range(at - len(copies), at):
            total = total + others[i]
    return total


def scattered(side, grads):
    count = len(grads)
    owners = (side, side, CORES)
    blocks = [(g.shape[0] // math.prod(owners), g.shape[1]) for g in grads]
    shaped = [g.reshape(owners + b) for g, b in zip(grads, blocks)]
    leads = [(side, side), (side, side), (side - 1, side), (side,), (side - 1,)]
    stages = 2 * side - 1
    out = pl.pallas_call(
        functools.partial(scatter_kernel, side, count),
        out_shape=[jax.ShapeDtypeStruct(b, jnp.bfloat16) for b in blocks] + [jax.ShapeDtypeStruct((8, 128), jnp.float32)],
        in_specs=[VMEM] * count,
        out_specs=[VMEM] * (count + 1),
        scratch_shapes=[pltpu.VMEM(lead + b, jnp.bfloat16) for lead in leads for b in blocks]
        + [
            pltpu.VMEM((3, 8, 128), jnp.float32),
            pltpu.VMEM((stages, 8, 128), jnp.float32),
            pltpu.SemaphoreType.DMA((count, stages)),
            pltpu.SemaphoreType.DMA((count, stages)),
            pltpu.SemaphoreType.DMA((stages,)),
            pltpu.SemaphoreType.DMA((stages,)),
        ],
        compiler_params=pltpu.CompilerParams(collective_id=1, has_side_effects=True, vmem_limit_bytes=60 << 20),
        name="scatter",
    )(*shaped)
    return out[:count], out[count]


def solution(mesh):
    side = math.isqrt(mesh.shape["dp"] // CORES)

    def step(x, dy, *arrays):
        weights, m, v = (arrays[i : i + 3] for i in (0, 3, 6))
        layers = weights[0].shape[0]
        whole = gathered(side, weights)
        fetched = [dict(zip(NAMES, whole[3 * n : 3 * n + 3], strict=True)) for n in range(layers)]
        h, kept = x[0], []
        for number in range(layers):
            kept.append(h)
            h = layer(h, fetched[number])
        by_h, grads = dy[0], []
        for number in reversed(range(layers)):
            _, back = jax.vjp(lambda w, h: layer(h, w), fetched[number], kept[number])
            by_w, by_h = back(by_h)
            grads = [by_w[name] for name in NAMES] + grads
        mine, squares = scattered(side, grads)
        gradients = [jnp.stack([mine[3 * n + i] for n in range(layers)]).astype(jnp.float32) for i in range(3)]
        count = mesh.shape["dp"] * sum(g.size for g in gradients)
        factor = jnp.minimum(1.0, 0.5 * lax.rsqrt(jnp.sum(squares) / count + 1e-30))
        new = [adamw(w.astype(jnp.float32), m, v, g * factor) for w, m, v, g in zip(weights, m, v, gradients, strict=True)]
        return tuple(one[which] for which in range(3) for one in new)

    states, cut = P(("rep", "dp"), None, None), P(None, "dp", None)
    return jax.shard_map(
        step,
        mesh=mesh,
        in_specs=(states, states) + (cut,) * 9,
        out_specs=(P("rep", "dp", None),) * 9,
        check_vma=False,
    )
```

```python
import functools
import math

import jax
import jax.numpy as jnp
from jax import lax
from jax.experimental import pallas as pl
from jax.experimental.pallas import tpu as pltpu
from jax.sharding import PartitionSpec as P

MESH = pl.DeviceIdType.MESH
CORES = 2
WIDE = 256
BLOCKS = 3
CHUNK = WIDE * BLOCKS
ROWS = 256
VMEM = pl.BlockSpec(memory_space=pltpu.VMEM)
HBM = pl.BlockSpec(memory_space=pl.ANY)
BF16, F32 = jnp.bfloat16, jnp.float32


def dot(a, b):
    return jnp.dot(a, b, preferred_element_type=F32)


def dot_t(a, b):
    return lax.dot_general(a, b, (((1,), (1,)), ((), ())), preferred_element_type=F32)


def adamw(w, m, v, g):
    m = 0.9 * m + 0.1 * g
    v = 0.95 * v + 0.05 * g * g
    step = m * lax.rsqrt(v + 1e-8) + 0.1 * w
    return (w - 0.02 * step).astype(BF16), m, v


class Place:
    def __init__(self, side):
        self.side = side
        me = lax.axis_index("dp")
        self.c = lax.rem(me, CORES)
        self.y = lax.rem(me // CORES, side)
        self.x = me // (CORES * side)

    def device(self, x, y, c):
        return {"dp": (x * self.side + y) * CORES + c}

    def partner(self):
        return self.device(self.x, self.y, 1 - self.c)

    def along(self, axis, k):
        if axis == "x":
            x = lax.rem(self.x + k + self.side, self.side)
            return x, self.device(x, self.y, self.c)
        y = lax.rem(self.y + k + self.side, self.side)
        return y, self.device(self.x, y, self.c)

    def others(self):
        return [self.partner()] + [self.along(a, k)[1] for a in "xy" for k in range(1, self.side)]

    def barrier(self):
        sem = pltpu.get_barrier_semaphore()
        for other in self.others():
            pl.semaphore_signal(sem, inc=1, device_id=other, device_id_type=MESH)
        pl.semaphore_wait(sem, len(self.others()))


def send(src, dst, sems, device):
    return pltpu.make_async_remote_copy(
        src_ref=src, dst_ref=dst, send_sem=sems[0], recv_sem=sems[1], device_id=device, device_id_type=MESH
    )


class Gather:
    STAGES = 5

    def __init__(self, place, whole, rows, cols, send_sems, recv_sems, first):
        p = place
        sems = [(send_sems.at[i], recv_sems.at[i]) for i in range(9)]
        second = "y" if first == "x" else "x"
        half = cols.size // 2
        halves = [pl.ds(cols.start, half), pl.ds(cols.start + half, half)]

        def block(i, cols):
            return whole.at[i, p.y, p.c, rows, cols] if first == "x" else whole.at[p.x, i, p.c, rows, cols]

        def line(i, cols):
            return whole.at[:, i, p.c, rows, cols] if first == "x" else whole.at[i, :, p.c, rows, cols]

        self.stages = []
        for axis, part, base in ((first, block, 0), (second, line, 4)):
            me = p.along(axis, 0)[0]
            (after, up), (before, down) = p.along(axis, 1), p.along(axis, -1)
            mine = part(me, cols)
            self.stages.append([(mine, sems[base], up), (mine, sems[base + 1], down)])
            self.stages.append([(part(before, halves[0]), sems[base + 2], up), (part(after, halves[1]), sems[base + 3], down)])
        self.stages.append([(whole.at[:, :, p.c, rows, cols], sems[8], p.partner())])

    def start(self, stage):
        for part, sems, device in self.stages[stage]:
            send(part, part, sems, device).start()

    def wait(self, stage):
        for part, sems, device in self.stages[stage]:
            send(part, part, sems, device).wait()


class Scatter:
    def __init__(self, place, refs, send_sems, recv_sems, first):
        p, s = place, place.side
        self.p, self.s, self.first, self.refs = p, s, first, refs
        mine, pair, paired, line, lined, last = refs
        sems = [(send_sems.at[i], recv_sems.at[i]) for i in range(2 * s - 1)]
        second = "y" if first == "x" else "x"
        self.stages = [[(mine.at[:, :, 1 - p.c], pair, sems[0], p.partner())], [], []]
        for k in range(1, s):
            there, device = p.along(first, k)
            part = paired.at[there] if first == "x" else paired.at[:, there]
            self.stages[1].append((part, line.at[k - 1], sems[k], device))
        for k in range(1, s):
            there, device = p.along(second, k)
            self.stages[2].append((lined.at[there], last.at[k - 1], sems[s - 1 + k], device))

    def start(self, stage):
        for copy in self.stages[stage]:
            send(*copy).start()

    def wait(self, stage):
        for copy in self.stages[stage]:
            send(*copy).wait()

    def _pair_sum(self, x, y):
        mine, pair = self.refs[:2]
        return mine[x, y, self.p.c].astype(F32) + pair[x, y].astype(F32)

    def _line_sum(self, i):
        p, line = self.p, self.refs[3]
        total = self._pair_sum(p.x, i) if self.first == "x" else self._pair_sum(i, p.y)
        for k in range(self.s - 1):
            total += line[k, i].astype(F32)
        return total

    def add(self, stage):
        s = self.s
        _, _, paired, _, lined, _ = self.refs
        if stage == 0:

            @pl.loop(0, s * s)
            def _(i):
                x, y = i // s, lax.rem(i, s)
                paired[x, y] = self._pair_sum(x, y).astype(BF16)

        else:

            @pl.loop(0, s)
            def _(i):
                lined[i] = self._line_sum(i).astype(BF16)

    def result(self, write):
        p, last = self.p, self.refs[5]
        total = self._line_sum(p.y if self.first == "x" else p.x)
        for k in range(self.s - 1):
            total += last[k].astype(F32)
        write(total.astype(BF16))


class ScatterRows:
    def __init__(self, place, refs, send_sems, recv_sems, owner):
        p, s = place, place.side
        self.p, self.s, self.refs, self.owner = p, s, refs, owner
        mine, pair, paired, line, lined, last = refs
        sems = [(send_sems.at[i], recv_sems.at[i]) for i in range(2 * s - 1)]
        self.first = [(mine.at[:, 1 - p.c], pair, sems[0], p.partner())]
        self.second = []
        for k in range(1, s):
            there, device = p.along("y", k)
            self.second.append((paired.at[there], line.at[k - 1], sems[k], device))
        self.last_sems = [sems[s - 1 + k] for k in range(1, s)]
        self.away = lax.rem(owner - p.x + s, s)

    def _last(self, k):
        lined, last = self.refs[4:]
        return send(lined, last.at[k - 1], self.last_sems[k - 1], self.p.device(self.owner, self.p.y, self.p.c))

    def start(self, stage):
        if stage < 2:
            for copy in (self.first, self.second)[stage]:
                send(*copy).start()
        else:
            for k in range(1, self.s):

                @pl.when(self.away == k)
                def _():
                    self._last(k).start()

    def wait(self, stage):
        if stage < 2:
            for copy in (self.first, self.second)[stage]:
                send(*copy).wait()
        else:
            for k in range(1, self.s):

                @pl.when(self.away == k)
                def _():
                    self._last(k).wait_send()

                @pl.when(self.away == 0)
                def _():
                    self._last(k).wait_recv()

    def _pair_sum(self, y):
        mine, pair = self.refs[:2]
        return mine[y, self.p.c].astype(F32) + pair[y].astype(F32)

    def _line_sum(self):
        total = self._pair_sum(self.p.y)
        for k in range(self.s - 1):
            total += self.refs[3][k].astype(F32)
        return total

    def add(self, stage):
        _, _, paired, _, lined, _ = self.refs
        if stage == 0:

            @pl.loop(0, self.s)
            def _(y):
                paired[y] = self._pair_sum(y).astype(BF16)

        else:
            lined[...] = self._line_sum().astype(BF16)

    def result(self, write):
        @pl.when(self.away == 0)
        def _():
            total = self._line_sum()
            for k in range(self.s - 1):
                total += self.refs[5][k].astype(F32)
            write(total.astype(BF16))


def fold(wide):
    rows, columns = wide.shape
    rows8 = wide.reshape(rows // 8, 8, columns).sum(0)
    total = rows8[:, :128]
    for i in range(128, columns, 128):
        total += rows8[:, i : i + 128]
    return total


def reduced(p, total, squares, others, send_sems, recv_sems):
    at = 0
    for stage, devices in enumerate(
        ([p.partner()], [p.along("y", k)[1] for k in range(1, p.side)], [p.along("x", k)[1] for k in range(1, p.side)])
    ):
        squares[stage] = total
        copies = []
        for device in devices:
            copies.append(send(squares.at[stage], others.at[at], (send_sems.at[at], recv_sems.at[at]), device))
            at += 1
        for copy in copies:
            copy.start()
        for copy in copies:
            copy.wait()
        for i in range(at - len(copies), at):
            total = total + others[i]
    return total


def rms(wide):
    return lax.rsqrt(jnp.mean(wide * wide, -1, keepdims=True) + 1e-6)


def kernel(side, x_in, dy_in, g_in, u_in, d_in, og, ou, od, norm, *scratch):
    (wg, wu, wd, a, a_t, b, b_t, h, acc, p3, squares, others, gg, gu, gd, pg, pu, pd, sg, su, sd, lg, lu, ld, mg, mu, md, eg, eu, ed) = scratch[:30]
    ag_send, ag_recv, rs_send, rs_recv, local, norm_send, norm_recv, free = scratch[30:]
    p = Place(side)
    layers, depth, hidden = wg.shape[0], a.shape[1], wg.shape[-1]
    tokens = a.shape[0]
    chunks = hidden // CHUNK
    steps = layers * chunks
    flat_g, flat_u = (w.reshape(layers, depth, hidden) for w in (wg, wu))
    flat_d = wd.reshape(layers, hidden, depth)

    def shards():
        for i, (shard, whole) in enumerate(((g_in, wg), (u_in, wu), (d_in, wd))):
            for n in range(layers):
                yield pltpu.make_async_copy(shard.at[n], whole.at[n, p.x, p.y, p.c], local.at[i * layers + n])

    def load(i):
        source, target = ((x_in, h), (dy_in, b))[i]
        return pltpu.make_async_copy(source.at[0], target, local.at[3 * layers + i])

    for copy in shards():
        copy.start()
    for i in range(2):
        load(i).start()

    pairs = []

    def pair(*units):
        made = []
        for whole, rows, cols, first in units:
            at = 2 * len(pairs) + len(made)
            made.append(Gather(p, whole, rows, cols, ag_send.at[at], ag_recv.at[at], first))
        pairs.append(made)

    def chunk_pair(n, j):
        rows, cols = pl.ds(0, g_in.shape[1]), pl.ds(j * CHUNK, CHUNK)
        pair((wg.at[n], rows, cols, "x"), (wu.at[n], rows, cols, "y"))

    def down_pairs(n):
        rows, cols = d_in.shape[1] // 2, depth // 2
        for k in range(2):
            pair(
                (wd.at[n], pl.ds(0, rows), pl.ds(k * cols, cols), "x"),
                (wd.at[n], pl.ds(rows, rows), pl.ds(k * cols, cols), "y"),
            )

    for n in range(layers):
        if n == layers - 1:
            down_pairs(n)
        for j in range(chunks):
            if n < layers - 1 and j == chunks - 1:
                down_pairs(n)
            chunk_pair(n, j)

    def gather_round(r):
        if r < len(pairs):
            for unit in pairs[r]:
                unit.start(0)
        for stage in range(Gather.STAGES):
            i = r - 1 - stage
            if 0 <= i < len(pairs):
                for unit in pairs[i]:
                    unit.wait(stage)
                    if stage + 1 < Gather.STAGES:
                        unit.start(stage + 1)

    def columns(j, n=None):
        if n is None:
            return pl.ds(pl.multiple_of(j * CHUNK, CHUNK), CHUNK)
        return pl.ds(pl.multiple_of(j * CHUNK + n * WIDE, WIDE), WIDE)

    def tiles(size, body):
        @pl.loop(0, tokens // size)
        def _(t):
            body(pl.ds(pl.multiple_of(t * size, size), size))

    def forward(n, j, slot):
        @pl.loop(0, BLOCKS)
        def _(i):
            gate, up = dot(a[...], flat_g[n, :, columns(j, i)]), dot(a[...], flat_u[n, :, columns(j, i)])
            p3[slot, :, columns(0, i)] = (jax.nn.silu(gate) * up).astype(BF16)

    def down(n, parts, more):
        @pl.loop(0, depth // WIDE)
        def _(i):
            cols = columns(0, i)
            y = sum(dot(p3[slot], flat_d[n, pl.ds(j * CHUNK, CHUNK), cols]) for j, slot in parts)
            if more:
                acc[:, cols] = y
            else:
                y = (acc[:, cols] + y).astype(BF16)
                h[:, cols] = h[:, cols] + y

    def norms(transposed):
        def body(rows):
            wide = h[rows, :].astype(F32)
            scaled = (wide * rms(wide)).astype(BF16)
            a[rows, :] = scaled
            if transposed:
                a_t[:, rows] = scaled.T

        tiles(ROWS, body)

    def transpose_b(rows):
        b_t[:, rows] = b[rows, :].T

    def backward(n, j, i):
        gate, up = dot(a[...], flat_g[n, :, columns(j, i)]), dot(a[...], flat_u[n, :, columns(j, i)])
        by_z = dot_t(b[...], flat_d[n, columns(j, i), :]).astype(BF16).astype(F32)
        s = jax.nn.sigmoid(gate)
        silu = gate * s
        cols = columns(0, i)
        p3[0, :, cols] = (silu * up).astype(BF16)
        p3[1, :, cols] = (by_z * up * (s + silu * (1 - s))).astype(BF16)
        p3[2, :, cols] = (by_z * silu).astype(BF16)

    def by_normed(n, j):
        @pl.loop(0, depth // WIDE)
        def _(i):
            rows = columns(0, i)
            acc[:, rows] += dot_t(p3[1], flat_g[n, rows, columns(j)]) + dot_t(p3[2], flat_u[n, rows, columns(j)])

    def by_states(rows):
        wide = h[rows, :].astype(F32)
        scale = rms(wide)
        by = acc[rows, :].astype(BF16).astype(F32)
        along = jnp.sum(by * wide, -1, keepdims=True) * (scale * scale * scale) * (1 / depth)
        new = b[rows, :] + (by * scale - wide * along).astype(BF16)
        b[rows, :] = new
        b_t[:, rows] = new.T

    flat_gg, flat_gu = (r.reshape(CORES, depth, CHUNK) for r in (gg, gu))
    flat_gd = gd.reshape(CORES, CHUNK, depth)

    def scatters(q):
        slot, j = lax.rem(q, 2), lax.rem(q, chunks)
        sems = [(rs_send.at[slot, i], rs_recv.at[slot, i]) for i in range(3)]
        at = lambda *refs: [r.at[slot] for r in refs]
        g = Scatter(p, (*at(gg, pg), sg, *at(lg), mg, *at(eg)), *sems[0], "x")
        u = Scatter(p, (*at(gu, pu), su, *at(lu), mu, *at(eu)), *sems[1], "y")
        d = ScatterRows(p, (*at(gd, pd), sd, *at(ld), md, *at(ed)), *sems[2], j)
        return g, u, d

    def finish(q):
        n, j = layers - 1 - q // chunks, lax.rem(q, chunks)
        g, u, d = scatters(q)

        def keep(out, *where):
            def write(total):
                out[where] = total
                wide = total.astype(F32)
                squares[3] = squares[3] + fold(wide * wide)

            return write

        for unit, write in ((g, keep(og, n, slice(None), columns(j))), (u, keep(ou, n, slice(None), columns(j))), (d, keep(od, n))):
            unit.wait(2)
            unit.result(write)

        @pl.when(q + 2 < steps)
        def _():
            for other in p.others():
                pl.semaphore_signal(free.at[lax.rem(q, 2)], inc=1, device_id=other, device_id_type=MESH)

    p.barrier()
    for copy in shards():
        copy.wait()
    last_rounds = Gather.STAGES - 2
    rounds = len(pairs) + Gather.STAGES
    done = 0
    for r in range(rounds - last_rounds):
        gather_round(r)
        if r == 0:
            load(0).wait()
            norms(False)
        elif r == 1:
            load(1).wait()
            tiles(ROWS, transpose_b)
            squares[3] = jnp.zeros_like(squares[3])
        ready = r - Gather.STAGES
        if 0 <= ready < chunks - 1:
            forward(0, ready, ready)
        elif ready == chunks:
            down(0, [(j, j) for j in range(chunks - 1)], True)
        elif ready == chunks + 1:
            forward(0, chunks - 1, 0)
            down(0, [(chunks - 1, 0)], False)
            norms(True)
            acc[...] = jnp.zeros_like(acc)

    @pl.loop(0, steps + 2)
    def _(q):
        n, j, slot = layers - 1 - q // chunks, lax.rem(q, chunks), lax.rem(q, 2)
        computes = q < steps
        sends = (q > 0) & (q <= steps)

        @pl.when(q == chunks)
        def _():
            tiles(ROWS, by_states)
            load(0).start()
            load(0).wait()
            norms(True)

        @pl.when(computes)
        def _():
            backward(n, j, 0)

        @pl.when(sends)
        def _():
            for unit in scatters(q - 1):
                unit.wait(0)
                unit.add(0)
                unit.start(1)

        @pl.when(q >= 2)
        def _():
            finish(q - 2)

        @pl.when(computes)
        def _():
            @pl.loop(1, BLOCKS)
            def _(i):
                backward(n, j, i)

        for k in range(last_rounds):

            @pl.when(q == k)
            def _():
                gather_round(rounds - last_rounds + k)

        @pl.when(computes & (q < chunks))
        def _():
            by_normed(n, j)

        @pl.when(computes)
        def _():
            g, u, _ = scatters(q)
            flat_gg[slot] = dot(a_t[...], p3[1]).astype(BF16)

            @pl.when(q >= 2)
            def _():
                pl.semaphore_wait(free.at[slot], len(p.others()))

            g.start(0)
            flat_gu[slot] = dot(a_t[...], p3[2]).astype(BF16)
            u.start(0)

        @pl.when(sends)
        def _():
            for unit in scatters(q - 1):
                unit.wait(1)
                unit.add(1)
                unit.start(2)

        @pl.when(computes)
        def _():
            flat_gd[slot] = dot(b_t[...], p3[0]).T.astype(BF16)
            scatters(q)[2].start(0)

    norm[...] = reduced(p, squares[3], squares, others, norm_send, norm_recv)


def gradients_of(side, x, dy, weights):
    w_gate, _, w_down = weights
    layers, rows, hidden = w_gate.shape
    rows_d, depth = w_down.shape[1:]
    tokens = x.shape[1]
    chunk, block, rest = (rows, CHUNK), (rows_d, depth), side - 1

    def whole(w):
        return pltpu.VMEM((layers, side, side, CORES) + w.shape[1:], BF16)

    def buffers(lead, lead_d):
        return [pltpu.VMEM(lead + chunk, BF16)] * 2 + [pltpu.VMEM(lead_d + block, BF16)]

    pairs = layers * (hidden // CHUNK + 2)
    stages = 2 * side - 1
    return pl.pallas_call(
        functools.partial(kernel, side),
        out_shape=[jax.ShapeDtypeStruct(w.shape, BF16) for w in weights] + [jax.ShapeDtypeStruct((8, 128), F32)],
        in_specs=[HBM] * 5,
        out_specs=[VMEM] * 4,
        scratch_shapes=[whole(w) for w in weights]
        + [
            pltpu.VMEM((tokens, depth), BF16),
            pltpu.VMEM((depth, tokens), BF16),
            pltpu.VMEM((tokens, depth), BF16),
            pltpu.VMEM((depth, tokens), BF16),
            pltpu.VMEM((tokens, depth), BF16),
            pltpu.VMEM((tokens, depth), F32),
            pltpu.VMEM((3, tokens, CHUNK), BF16),
            pltpu.VMEM((4, 8, 128), F32),
            pltpu.VMEM((stages, 8, 128), F32),
        ]
        + buffers((2, side, side, CORES), (2, side, CORES))
        + buffers((2, side, side), (2, side))
        + buffers((side, side), (side,))
        + buffers((2, rest, side), (2, rest))
        + buffers((side,), ())
        + buffers((2, rest), (2, rest))
        + [
            pltpu.SemaphoreType.DMA((2 * pairs, 9)),
            pltpu.SemaphoreType.DMA((2 * pairs, 9)),
            pltpu.SemaphoreType.DMA((2, 3, stages)),
            pltpu.SemaphoreType.DMA((2, 3, stages)),
            pltpu.SemaphoreType.DMA((3 * layers + 2,)),
            pltpu.SemaphoreType.DMA((stages,)),
            pltpu.SemaphoreType.DMA((stages,)),
            pltpu.SemaphoreType.REGULAR((2,)),
        ],
        compiler_params=pltpu.CompilerParams(collective_id=0, has_side_effects=True, vmem_limit_bytes=67043328),
        name="gradients",
    )(x, dy, *weights)


def solution(mesh):
    side = math.isqrt(mesh.shape["dp"] // CORES)

    def step(x, dy, *arrays):
        weights, m, v = (arrays[i : i + 3] for i in (0, 3, 6))
        *gradients, squares = gradients_of(side, x, dy, weights)
        count = mesh.shape["dp"] * sum(g.size for g in gradients)
        factor = jnp.minimum(1.0, 0.5 * lax.rsqrt(jnp.sum(squares) / count + 1e-30))
        new = [adamw(w.astype(F32), m, v, g.astype(F32) * factor) for w, m, v, g in zip(weights, m, v, gradients, strict=True)]
        return tuple(one[which] for which in range(3) for one in new)

    states, cut = P(("rep", "dp"), None, None), P(None, "dp", None)
    return jax.shard_map(
        step,
        mesh=mesh,
        in_specs=(states, states) + (cut,) * 9,
        out_specs=(P("rep", "dp", None),) * 9,
        check_vma=False,
    )
```

```python
import functools
import math

import jax
import jax.numpy as jnp
from jax import lax
from jax.experimental import pallas as pl
from jax.experimental.pallas import tpu as pltpu
from jax.sharding import PartitionSpec as P

MESH = pl.DeviceIdType.MESH
CORES = 2
WIDE = 256
BLOCKS = 3
CHUNK = WIDE * BLOCKS
TALL = 512
ROWS = 256
EARLY = 2
WINDOW = 8
VMEM = pl.BlockSpec(memory_space=pltpu.VMEM)
HBM = pl.BlockSpec(memory_space=pl.ANY)
BF16, F32 = jnp.bfloat16, jnp.float32


def dot(a, b):
    return jnp.dot(a, b, preferred_element_type=F32)


def dot_t(a, b):
    return lax.dot_general(a, b, (((1,), (1,)), ((), ())), preferred_element_type=F32)


def adamw(w, m, v, g):
    m = 0.9 * m + 0.1 * g
    v = 0.95 * v + 0.05 * g * g
    step = m * lax.rsqrt(v + 1e-8) + 0.1 * w
    return (w - 0.02 * step).astype(BF16), m, v


class Place:
    def __init__(self, side):
        self.side = side
        me = lax.axis_index("dp")
        self.c = lax.rem(me, CORES)
        self.y = lax.rem(me // CORES, side)
        self.x = me // (CORES * side)

    def device(self, x, y, c):
        return {"dp": (x * self.side + y) * CORES + c}

    def partner(self):
        return self.device(self.x, self.y, 1 - self.c)

    def along(self, axis, k):
        if axis == "x":
            x = lax.rem(self.x + k + self.side, self.side)
            return x, self.device(x, self.y, self.c)
        y = lax.rem(self.y + k + self.side, self.side)
        return y, self.device(self.x, y, self.c)

    def others(self):
        return [self.partner()] + [self.along(a, k)[1] for a in "xy" for k in range(1, self.side)]

    def slanted(self):
        return [self.device(self.x, self.along("y", k)[0], 1 - self.c) for k in range(1, self.side)]

    def barrier(self):
        sem = pltpu.get_barrier_semaphore()
        everyone = self.others() + self.slanted()
        for other in everyone:
            pl.semaphore_signal(sem, inc=1, device_id=other, device_id_type=MESH)
        pl.semaphore_wait(sem, len(everyone))


def send(src, dst, sems, device):
    return pltpu.make_async_remote_copy(
        src_ref=src, dst_ref=dst, send_sem=sems[0], recv_sem=sems[1], device_id=device, device_id_type=MESH
    )


class Gather:
    def __init__(self, place, whole, rows, cols, send_sems, recv_sems, first):
        p = place
        sems = [(send_sems.at[i], recv_sems.at[i]) for i in range(9)]
        second = "y" if first == "x" else "x"
        half = cols.size // 2
        halves = [pl.ds(cols.start, half), pl.ds(cols.start + half, half)]

        def block(i, cols):
            return whole.at[i, p.y, p.c, rows, cols] if first == "x" else whole.at[p.x, i, p.c, rows, cols]

        def line(i, cols):
            return whole.at[:, i, p.c, rows, cols] if first == "x" else whole.at[i, :, p.c, rows, cols]

        self.stages = []
        for axis, part, base in ((first, block, 0), (second, line, 4)):
            me = p.along(axis, 0)[0]
            (after, up), (before, down) = p.along(axis, 1), p.along(axis, -1)
            mine = part(me, cols)
            self.stages.append([(mine, sems[base], up), (mine, sems[base + 1], down)])
            self.stages.append([(part(before, halves[0]), sems[base + 2], up), (part(after, halves[1]), sems[base + 3], down)])
        self.stages.append([(whole.at[:, :, p.c, rows, cols], sems[8], p.partner())])

    def start(self, stage):
        for part, sems, device in self.stages[stage]:
            send(part, part, sems, device).start()

    def wait(self, stage):
        for part, sems, device in self.stages[stage]:
            send(part, part, sems, device).wait()


class Scatter:
    def __init__(self, place, refs, send_sems, recv_sems, first):
        p, s = place, place.side
        self.p, self.s, self.first, self.refs = p, s, first, refs
        mine, pair, paired, line, lined, last = refs
        sems = [(send_sems.at[i], recv_sems.at[i]) for i in range(2 * s - 1)]
        second = "y" if first == "x" else "x"
        self.stages = [[(mine.at[:, :, 1 - p.c], pair, sems[0], p.partner())], [], []]
        for k in range(1, s):
            there, device = p.along(first, k)
            part = paired.at[there] if first == "x" else paired.at[:, there]
            self.stages[1].append((part, line.at[k - 1], sems[k], device))
        for k in range(1, s):
            there, device = p.along(second, k)
            self.stages[2].append((lined.at[there], last.at[k - 1], sems[s - 1 + k], device))

    def start(self, stage):
        for copy in self.stages[stage]:
            send(*copy).start()

    def wait(self, stage):
        for copy in self.stages[stage]:
            send(*copy).wait()

    def _pair_sum(self, x, y):
        mine, pair = self.refs[:2]
        return mine[x, y, self.p.c].astype(F32) + pair[x, y].astype(F32)

    def _line_sum(self, i):
        p, line = self.p, self.refs[3]
        total = self._pair_sum(p.x, i) if self.first == "x" else self._pair_sum(i, p.y)
        for k in range(self.s - 1):
            total += line[k, i].astype(F32)
        return total

    def add(self, stage):
        s = self.s
        _, _, paired, _, lined, _ = self.refs
        if stage == 0:

            @pl.loop(0, s * s, unroll=4)
            def _(i):
                x, y = i // s, lax.rem(i, s)
                paired[x, y] = self._pair_sum(x, y).astype(BF16)

        else:

            @pl.loop(0, s, unroll=True)
            def _(i):
                lined[i] = self._line_sum(i).astype(BF16)

    def result(self, write):
        p, last = self.p, self.refs[5]
        total = self._line_sum(p.y if self.first == "x" else p.x)
        for k in range(self.s - 1):
            total += last[k].astype(F32)
        write(total.astype(BF16))


class ScatterRows:
    def __init__(self, place, refs, send_sems, recv_sems, owner):
        p, s = place, place.side
        self.p, self.s, self.refs, self.owner = p, s, refs, owner
        mine, pair, paired, line, lined, last = refs
        sems = [(send_sems.at[i], recv_sems.at[i]) for i in range(2 * s - 1)]
        self.first = [(mine.at[:, 1 - p.c], pair, sems[0], p.partner())]
        self.second = []
        for k in range(1, s):
            there, device = p.along("y", k)
            self.second.append((paired.at[there], line.at[k - 1], sems[k], device))
        self.last_sems = [sems[s - 1 + k] for k in range(1, s)]
        self.away = lax.rem(owner - p.x + s, s)

    def _last(self, k):
        lined, last = self.refs[4:]
        return send(lined, last.at[k - 1], self.last_sems[k - 1], self.p.device(self.owner, self.p.y, self.p.c))

    def start(self, stage):
        if stage < 2:
            for copy in (self.first, self.second)[stage]:
                send(*copy).start()
        else:
            for k in range(1, self.s):

                @pl.when(self.away == k)
                def _():
                    self._last(k).start()

    def wait(self, stage):
        if stage < 2:
            for copy in (self.first, self.second)[stage]:
                send(*copy).wait()
        else:
            for k in range(1, self.s):

                @pl.when(self.away == k)
                def _():
                    self._last(k).wait_send()

                @pl.when(self.away == 0)
                def _():
                    self._last(k).wait_recv()

    def _pair_sum(self, y):
        mine, pair = self.refs[:2]
        return mine[y, self.p.c].astype(F32) + pair[y].astype(F32)

    def _line_sum(self):
        total = self._pair_sum(self.p.y)
        for k in range(self.s - 1):
            total += self.refs[3][k].astype(F32)
        return total

    def add(self, stage):
        _, _, paired, _, lined, _ = self.refs
        if stage == 0:

            @pl.loop(0, self.s, unroll=True)
            def _(y):
                paired[y] = self._pair_sum(y).astype(BF16)

        else:
            lined[...] = self._line_sum().astype(BF16)

    def result(self, write):
        @pl.when(self.away == 0)
        def _():
            total = self._line_sum()
            for k in range(self.s - 1):
                total += self.refs[5][k].astype(F32)
            write(total.astype(BF16))


def fold(wide):
    rows, columns = wide.shape
    rows8 = wide.reshape(rows // 8, 8, columns).sum(0)
    total = rows8[:, :128]
    for i in range(128, columns, 128):
        total += rows8[:, i : i + 128]
    return total


def reduced(p, total, squares, others, send_sems, recv_sems):
    at = 0
    along = lambda axis: [p.along(axis, k)[1] for k in range(1, p.side)]
    for stage, devices in enumerate(([p.partner()] + along("y") + p.slanted(), along("x"))):
        squares[stage] = total
        copies = []
        for device in devices:
            copies.append((squares.at[stage], others.at[at], (send_sems.at[at], recv_sems.at[at]), device))
            at += 1
        for copy in copies:
            send(*copy).start()
        for copy in copies:
            send(*copy).wait()
        for i in range(at - len(copies), at):
            total = total + others[i]
    return total


def rms(wide):
    return lax.rsqrt(jnp.mean(wide * wide, -1, keepdims=True) + 1e-6)


def kernel(side, count, x_in, dy_in, g_in, u_in, d_in, *refs):
    outs, (wg, wu, wd, a, a_t, b, b_t, h, acc, p3, squares, others), refs = refs[:3], refs[3:15], refs[15:]
    (gg, gu, gd, pg, pu, pd, sg, su, sd, lg, lu, ld, mg, mu, md, eg, eu, ed), refs = refs[:18], refs[18:]
    ag_send, ag_recv, rs_send, rs_recv, local, norm_send, norm_recv, free = refs
    p = Place(side)
    layers, tokens, depth = a.shape
    hidden = wg.shape[-1]
    chunks = hidden // CHUNK
    steps = layers * chunks
    flat_g, flat_u = (w.reshape(layers, depth, hidden) for w in (wg, wu))
    flat_d = wd.reshape(layers, hidden, depth)

    def shards():
        for i, (shard, whole) in enumerate(((g_in, wg), (u_in, wu), (d_in, wd))):
            for n in range(layers):
                yield pltpu.make_async_copy(shard.at[n], whole.at[n, p.x, p.y, p.c], local.at[i * layers + n])

    def load(i):
        source, target = ((x_in, h), (dy_in, b))[i]
        return pltpu.make_async_copy(source.at[0], target, local.at[3 * layers + i])

    for copy in shards():
        copy.start()
    for i in range(2):
        load(i).start()

    pairs = []

    def pair(*units):
        made = []
        for whole, rows, cols, first in units:
            at = 2 * (len(pairs) % WINDOW) + len(made)
            made.append(Gather(p, whole, rows, cols, ag_send.at[at], ag_recv.at[at], first))
        pairs.append(made)

    def chunk_pair(n, j):
        rows, cols = pl.ds(0, g_in.shape[1]), pl.ds(j * CHUNK, CHUNK)
        pair((wg.at[n], rows, cols, "x"), (wu.at[n], rows, cols, "y"))

    def down_pairs(n):
        rows, cols = d_in.shape[1] // 2, depth // 2
        for k in range(2):
            pair(
                (wd.at[n], pl.ds(0, rows), pl.ds(k * cols, cols), "x"),
                (wd.at[n], pl.ds(rows, rows), pl.ds(k * cols, cols), "y"),
            )

    for n in range(layers):
        if n == layers - 1:
            down_pairs(n)
        for j in range(chunks):
            if n < layers - 1 and j == chunks // 2:
                down_pairs(n)
            chunk_pair(n, j)

    begins = [0, 1, 1, 2, 2, *range(3, len(pairs) - 2)]
    ends = [begin + len(units[0].stages) for begin, units in zip(begins, pairs)]

    def gather_round(r):
        for begin, end, units in reversed(list(zip(begins, ends, pairs))):
            for unit in units:
                if begin < r <= end:
                    unit.wait(r - begin - 1)
                if begin <= r < end:
                    unit.start(r - begin)

    def columns(j, n=None):
        if n is None:
            return pl.ds(pl.multiple_of(j * CHUNK, CHUNK), CHUNK)
        return pl.ds(pl.multiple_of(j * CHUNK + n * WIDE, WIDE), WIDE)

    def tiles(size, body):
        @pl.loop(0, tokens // size)
        def _(t):
            body(pl.ds(pl.multiple_of(t * size, size), size))

    bands = [pl.ds(i, TALL) for i in range(0, tokens, TALL)]

    def forward(n, j, slot):
        for i in range(BLOCKS):
            for rows in bands:
                gate, up = dot(a[n, rows, :], flat_g[n, :, columns(j, i)]), dot(a[n, rows, :], flat_u[n, :, columns(j, i)])
                p3[slot, rows, columns(0, i)] = (jax.nn.silu(gate) * up).astype(BF16)

    def down(n, parts, more):
        for i in range(depth // WIDE):
            cols = columns(0, i)
            for rows in bands:
                y = sum(dot(p3[slot, rows, :], flat_d[n, pl.ds(j * CHUNK, CHUNK), cols]) for j, slot in parts)
                if more:
                    acc[rows, cols] = y
                else:
                    y = (acc[rows, cols] + y).astype(BF16)
                    h[rows, cols] = h[rows, cols] + y

    def norms(n):
        def body(rows):
            wide = h[rows, :].astype(F32)
            scaled = (wide * rms(wide)).astype(BF16)
            a[n, rows, :] = scaled
            a_t[n, :, rows] = scaled.T

        tiles(ROWS, body)

    def transpose_b(rows):
        b_t[:, rows] = b[rows, :].T

    def backward(n, j):
        for i in range(BLOCKS):
            for rows in bands:
                gate, up = dot(a[n, rows, :], flat_g[n, :, columns(j, i)]), dot(a[n, rows, :], flat_u[n, :, columns(j, i)])
                by_z = dot_t(b[rows, :], flat_d[n, columns(j, i), :]).astype(BF16).astype(F32)
                s = jax.nn.sigmoid(gate)
                silu = gate * s
                cols = columns(0, i)
                p3[0, rows, cols] = (silu * up).astype(BF16)
                p3[1, rows, cols] = (by_z * up * (s + silu * (1 - s))).astype(BF16)
                p3[2, rows, cols] = (by_z * silu).astype(BF16)

    def by_normed(n, j):
        for i in range(depth // WIDE):
            cols = columns(0, i)
            for rows in bands:
                by_gate, by_up = dot_t(p3[1, rows, :], flat_g[n, cols, columns(j)]), dot_t(p3[2, rows, :], flat_u[n, cols, columns(j)])
                acc[rows, cols] += by_gate + by_up

    def by_states(rows):
        wide = h[rows, :].astype(F32)
        scale = rms(wide)
        by = acc[rows, :].astype(BF16).astype(F32)
        along = jnp.sum(by * wide, -1, keepdims=True) * (scale * scale * scale) * (1 / depth)
        new = b[rows, :] + (by * scale - wide * along).astype(BF16)
        b[rows, :] = new
        b_t[:, rows] = new.T

    flat_gg, flat_gu = (r.reshape(CORES, depth, CHUNK) for r in (gg, gu))
    flat_gd = gd.reshape(CORES, CHUNK, depth)

    def scatters(q):
        slot, j = lax.rem(q, 2), lax.rem(q, chunks)
        sems = [(rs_send.at[slot, i], rs_recv.at[slot, i]) for i in range(3)]
        at = lambda *refs: [r.at[slot] for r in refs]
        g = Scatter(p, (*at(gg, pg), sg, *at(lg), mg, *at(eg)), *sems[0], "x")
        u = Scatter(p, (*at(gu, pu), su, *at(lu), mu, *at(eu)), *sems[1], "y")
        d = ScatterRows(p, (*at(gd, pd), sd, *at(ld), md, *at(ed)), *sems[2], j)
        return g, u, d

    def finish(q):
        n, j = layers - 1 - q // chunks, lax.rem(q, chunks)
        g, u, d = scatters(q)

        def keep(out, *where):
            def write(total):
                wide = total.astype(F32)
                out[where] = wide
                squares[3] = squares[3] + fold(wide * wide)

            return write

        og, ou, od = outs
        for unit, write in ((g, keep(og, n, slice(None), columns(j))), (u, keep(ou, n, slice(None), columns(j))), (d, keep(od, n))):
            unit.wait(2)
            unit.result(write)

        @pl.when(q + 2 < steps)
        def _():
            for other in p.others():
                pl.semaphore_signal(free.at[lax.rem(q, 2)], inc=1, device_id=other, device_id_type=MESH)

    p.barrier()
    for copy in shards():
        copy.wait()
    starts = ends[len(pairs) - chunks]
    half = chunks // 2

    def last_down():
        down(0, [(j, j - half + 1) for j in range(half, chunks)], False)
        norms(1)
        acc[...] = jnp.zeros_like(acc)

    queue = [(j, functools.partial(forward, 0, j, j)) for j in range(half)]
    queue += [(half + 1, functools.partial(down, 0, [(j, j) for j in range(half)], True))]
    queue += [(j + 2, functools.partial(forward, 0, j, j - half + 1)) for j in range(half, chunks)]
    queue += [(chunks + 1, last_down)]
    work, at = {}, -1
    for needs, piece in queue:
        at = max(at + 1, ends[needs])
        work[at] = piece
    starts = max(starts, at)
    for r in range(starts + 1):
        gather_round(r)
        if r == 0:
            load(0).wait()
            norms(0)
        elif r == 1:
            load(1).wait()
            tiles(ROWS, transpose_b)
            squares[3] = jnp.zeros_like(squares[3])
        if r in work:
            work[r]()

    def by_weights(n, slot):
        by_gate, by_up = dot(a_t[n], p3[1]), dot(a_t[n], p3[2])
        flat_gg[slot] = by_gate.astype(BF16)
        flat_gu[slot] = by_up.astype(BF16)

    def by_down(slot):
        flat_gd[slot] = dot(b_t[...], p3[0]).T.astype(BF16)

    def advance(units, stage):
        for unit in units:
            unit.wait(stage)
            unit.add(stage)
            unit.start(stage + 1)

    def rs0(q):
        advance(scatters(q)[:2], 0)

    def rs1(q):
        g, u, d = scatters(q)
        advance((g, u), 1)

    def rs3(q):
        advance(scatters(q)[2:], 1)

    def rs2(q):
        advance(scatters(q)[2:], 0)

    def transition():
        tiles(ROWS, by_states)

    @pl.loop(0, steps + 2)
    def _(q):
        n, j, slot = layers - 1 - q // chunks, lax.rem(q, chunks), lax.rem(q, 2)
        computes = q < steps
        follows = (q > 0) & (q <= steps)

        @pl.when(q == chunks)
        def _():
            transition()

        @pl.when(computes)
        def _():
            backward(n, j)

        @pl.when(follows)
        def _():
            rs0(q - 1)

        @pl.when(q >= 2)
        def _():
            finish(q - 2)

        @pl.when(computes & (q < chunks))
        def _():
            by_normed(n, j)

        for k in range(ends[-1] - starts):

            @pl.when(q == k)
            def _():
                gather_round(starts + 1 + k)

        @pl.when(computes)
        def _():
            by_down(slot)

            @pl.when(q >= 2)
            def _():
                pl.semaphore_wait(free.at[slot], len(p.others()))

            scatters(q)[2].start(0)

        @pl.when(follows)
        def _():
            rs3(q - 1)

        @pl.when(computes)
        def _():
            by_weights(n, slot)
            for unit in scatters(q)[:2]:
                unit.start(0)
            rs2(q)

        @pl.when(follows)
        def _():
            rs1(q - 1)

    total = jnp.sum(reduced(p, squares[3], squares, others, norm_send, norm_recv), keepdims=True)
    factor = jnp.minimum(1.0, 0.5 * lax.rsqrt(total / count + 1e-30))
    for out in outs:
        out[...] = out[...] * factor.reshape(1, 1, 1)


def gradients_of(side, x, dy, weights):
    w_gate, _, w_down = weights
    layers, rows, hidden = w_gate.shape
    rows_d, depth = w_down.shape[1:]
    tokens = x.shape[1]
    chunk, block, rest = (rows, CHUNK), (rows_d, depth), side - 1

    def whole(w):
        return pltpu.VMEM((layers, side, side, CORES) + w.shape[1:], BF16)

    def buffers(lead, lead_d):
        return [pltpu.VMEM(lead + chunk, BF16)] * 2 + [pltpu.VMEM(lead_d + block, BF16)]

    stages = 2 * side - 1
    sums = 3 * side - 2
    count = side * side * CORES * sum(w.size for w in weights)
    return pl.pallas_call(
        functools.partial(kernel, side, count),
        out_shape=[jax.ShapeDtypeStruct(w.shape, F32) for w in weights],
        in_specs=[HBM] * 5,
        out_specs=[VMEM] * 3,
        scratch_shapes=[whole(w) for w in weights]
        + [
            pltpu.VMEM((layers, tokens, depth), BF16),
            pltpu.VMEM((layers, depth, tokens), BF16),
            pltpu.VMEM((tokens, depth), BF16),
            pltpu.VMEM((depth, tokens), BF16),
            pltpu.VMEM((tokens, depth), BF16),
            pltpu.VMEM((tokens, depth), F32),
            pltpu.VMEM((3, tokens, CHUNK), BF16),
            pltpu.VMEM((4, 8, 128), F32),
            pltpu.VMEM((sums, 8, 128), F32),
        ]

        + buffers((2, side, side, CORES), (2, side, CORES))
        + buffers((2, side, side), (2, side))
        + buffers((side, side), (side,))
        + buffers((2, rest, side), (2, rest))
        + buffers((side,), ())
        + buffers((2, rest), (2, rest))
        + [
            pltpu.SemaphoreType.DMA((2 * WINDOW, 9)),
            pltpu.SemaphoreType.DMA((2 * WINDOW, 9)),
            pltpu.SemaphoreType.DMA((2, 3, stages)),
            pltpu.SemaphoreType.DMA((2, 3, stages)),
            pltpu.SemaphoreType.DMA((3 * layers + 2,)),
            pltpu.SemaphoreType.DMA((sums,)),
            pltpu.SemaphoreType.DMA((sums,)),
            pltpu.SemaphoreType.REGULAR((2,)),
        ],
        compiler_params=pltpu.CompilerParams(collective_id=0, has_side_effects=True, vmem_limit_bytes=67043328),
        name="gradients",
    )(x, dy, *weights)


def solution(mesh):
    side = math.isqrt(mesh.shape["dp"] // CORES)

    def step(x, dy, *arrays):
        weights, m, v = (arrays[i : i + 3] for i in (0, 3, 6))
        gradients = gradients_of(side, x, dy, weights)
        new = [adamw(w.astype(F32), m, v, g) for w, m, v, g in zip(weights, m, v, gradients, strict=True)]
        return tuple(one[which] for which in range(3) for one in new)

    states, cut = P(("rep", "dp"), None, None), P(None, "dp", None)
    return jax.shard_map(
        step,
        mesh=mesh,
        in_specs=(states, states) + (cut,) * 9,
        out_specs=(P("rep", "dp", None),) * 9,
        check_vma=False,
    )
```

```python
import functools
import math

import jax
import jax.numpy as jnp
from jax import lax
from jax.experimental import pallas as pl
from jax.experimental.pallas import tpu as pltpu
from jax.sharding import PartitionSpec as P

MESH = pl.DeviceIdType.MESH
CORES = 2
WIDE = 256
BLOCKS = 3
CHUNK = WIDE * BLOCKS
GATHER_STEPS = 5
SCATTER_STEPS = 3
TALL = 512
ROWS = 256
EARLY = 2
WINDOW = 8
VMEM = pl.BlockSpec(memory_space=pltpu.VMEM)
HBM = pl.BlockSpec(memory_space=pl.ANY)
BF16, F32 = jnp.bfloat16, jnp.float32


def dot(a, b):
    return jnp.dot(a, b, preferred_element_type=F32)


def dot_t(a, b):
    return lax.dot_general(a, b, (((1,), (1,)), ((), ())), preferred_element_type=F32)


def adamw(w, m, v, g):
    m = 0.9 * m + 0.1 * g
    v = 0.95 * v + 0.05 * g * g
    step = m * lax.rsqrt(v + 1e-8) + 0.1 * w
    return (w - 0.02 * step).astype(BF16), m, v


class Place:
    def __init__(self, side):
        self.side = side
        me = lax.axis_index("dp")
        self.c = lax.rem(me, CORES)
        self.y = lax.rem(me // CORES, side)
        self.x = me // (CORES * side)

    def device(self, x, y, c):
        return {"dp": (x * self.side + y) * CORES + c}

    def partner(self):
        return self.device(self.x, self.y, 1 - self.c)

    def along(self, axis, k):
        if axis == "x":
            x = lax.rem(self.x + k + self.side, self.side)
            return x, self.device(x, self.y, self.c)
        y = lax.rem(self.y + k + self.side, self.side)
        return y, self.device(self.x, y, self.c)

    def others(self):
        return [self.partner()] + [self.along(a, k)[1] for a in "xy" for k in range(1, self.side)]

    def near(self):
        ys = [self.along("y", k)[0] for k in range(self.side)]
        return [self.partner()] + [self.device(self.x, y, c) for y in ys[1:] for c in (self.c, 1 - self.c)]

    def barrier(self):
        sem = pltpu.get_barrier_semaphore()
        greeted = self.near() + [self.along("x", k)[1] for k in range(1, self.side)]
        for other in greeted:
            pl.semaphore_signal(sem, inc=1, device_id=other, device_id_type=MESH)
        pl.semaphore_wait(sem, len(greeted))


def send(src, dst, sems, device):
    return pltpu.make_async_remote_copy(
        src_ref=src, dst_ref=dst, send_sem=sems[0], recv_sem=sems[1], device_id=device, device_id_type=MESH
    )


class Gather:
    def __init__(self, place, whole, rows, cols, send_sems, recv_sems, first):
        p = place
        sems = [(send_sems.at[i], recv_sems.at[i]) for i in range(GATHER_STEPS)]
        second = "y" if first == "x" else "x"
        half = cols.size // 2
        halves = [pl.ds(cols.start, half), pl.ds(cols.start + half, half)]

        def block(i, cols):
            return whole.at[i, p.y, p.c, rows, cols] if first == "x" else whole.at[p.x, i, p.c, rows, cols]

        def line(i, cols):
            return whole.at[:, i, p.c, rows, cols] if first == "x" else whole.at[i, :, p.c, rows, cols]

        self.stages = []
        both = pl.ds(0, 2)
        for axis, part in ((first, block), (second, line)):
            me = p.along(axis, 0)[0]
            (after, up), (before, down) = p.along(axis, 1), p.along(axis, -1)
            mine = part(me, cols)
            self.stages.append(([(mine, up), (mine, down)], part(both, cols)))
            self.stages.append(([(part(before, halves[0]), up), (part(after, halves[1]), down)], part(both, halves[0])))
        plane = whole.at[:, :, p.c, rows, cols]
        self.stages.append(([(plane, p.partner())], plane))
        self.sems, self.partner = sems, p.partner()

    def start(self, stage):
        for part, device in self.stages[stage][0]:
            send(part, part, self.sems[stage], device).start()

    def wait(self, stage):
        total = self.stages[stage][1]
        send(total, total, self.sems[stage], self.partner).wait()


class Scatter:
    def __init__(self, place, refs, send_sems, recv_sems, first):
        p, s = place, place.side
        self.p, self.s, self.first, self.refs = p, s, first, refs
        mine, pair, paired, line, lined, last = refs
        self.sems = [(send_sems.at[i], recv_sems.at[i]) for i in range(SCATTER_STEPS)]
        second = "y" if first == "x" else "x"
        self.totals = pair, line, last
        self.stages = [[(mine.at[:, :, 1 - p.c], pair, p.partner())], [], []]
        for k in range(1, s):
            there, device = p.along(first, k)
            part = paired.at[there] if first == "x" else paired.at[:, there]
            self.stages[1].append((part, line.at[k - 1], device))
        for k in range(1, s):
            there, device = p.along(second, k)
            self.stages[2].append((lined.at[there], last.at[k - 1], device))

    def start(self, stage):
        for src, dst, device in self.stages[stage]:
            send(src, dst, self.sems[stage], device).start()

    def wait(self, stage):
        total = self.totals[stage]
        send(total, total, self.sems[stage], self.p.partner()).wait()

    def _pair_sum(self, x, y):
        mine, pair = self.refs[:2]
        return mine[x, y, self.p.c].astype(F32) + pair[x, y].astype(F32)

    def _line_sum(self, i):
        p, line = self.p, self.refs[3]
        total = self._pair_sum(p.x, i) if self.first == "x" else self._pair_sum(i, p.y)
        for k in range(self.s - 1):
            total += line[k, i].astype(F32)
        return total

    def add(self, stage):
        s = self.s
        _, _, paired, _, lined, _ = self.refs
        if stage == 0:

            @pl.loop(0, s * s, unroll=4)
            def _(i):
                x, y = i // s, lax.rem(i, s)
                paired[x, y] = self._pair_sum(x, y).astype(BF16)

        else:

            @pl.loop(0, s, unroll=True)
            def _(i):
                lined[i] = self._line_sum(i).astype(BF16)

    def result(self, write):
        p, last = self.p, self.refs[5]
        total = self._line_sum(p.y if self.first == "x" else p.x)
        for k in range(self.s - 1):
            total += last[k].astype(F32)
        write(total.astype(BF16))


class ScatterRows:
    def __init__(self, place, refs, send_sems, recv_sems, owner):
        p, s = place, place.side
        self.p, self.s, self.refs, self.owner = p, s, refs, owner
        mine, pair, paired, line, lined, last = refs
        self.sems = [(send_sems.at[i], recv_sems.at[i]) for i in range(SCATTER_STEPS)]
        self.totals = pair, line, last
        self.first = [(mine.at[:, 1 - p.c], pair, p.partner())]
        self.second = []
        for k in range(1, s):
            there, device = p.along("y", k)
            self.second.append((paired.at[there], line.at[k - 1], device))
        self.away = lax.rem(owner - p.x + s, s)

    def _last(self, k):
        lined, last = self.refs[4:]
        return send(lined, last.at[k - 1], self.sems[2], self.p.device(self.owner, self.p.y, self.p.c))

    def start(self, stage):
        if stage < 2:
            for src, dst, device in (self.first, self.second)[stage]:
                send(src, dst, self.sems[stage], device).start()
        else:
            for k in range(1, self.s):

                @pl.when(self.away == k)
                def _():
                    self._last(k).start()

    def wait(self, stage):
        total = self.totals[stage]
        whole = lambda: send(total, total, self.sems[stage], self.p.partner())
        if stage < 2:
            whole().wait()
        else:

            @pl.when(self.away > 0)
            def _():
                self._last(1).wait_send()

            @pl.when(self.away == 0)
            def _():
                whole().wait_recv()

    def _pair_sum(self, y):
        mine, pair = self.refs[:2]
        return mine[y, self.p.c].astype(F32) + pair[y].astype(F32)

    def _line_sum(self):
        total = self._pair_sum(self.p.y)
        for k in range(self.s - 1):
            total += self.refs[3][k].astype(F32)
        return total

    def add(self, stage):
        _, _, paired, _, lined, _ = self.refs
        if stage == 0:

            @pl.loop(0, self.s, unroll=True)
            def _(y):
                paired[y] = self._pair_sum(y).astype(BF16)

        else:
            lined[...] = self._line_sum().astype(BF16)

    def result(self, write):
        @pl.when(self.away == 0)
        def _():
            total = self._line_sum()
            for k in range(self.s - 1):
                total += self.refs[5][k].astype(F32)
            write(total.astype(BF16))


def fold(wide):
    rows, columns = wide.shape
    rows8 = wide.reshape(rows // 8, 8, columns).sum(0)
    total = rows8[:, :128]
    for i in range(128, columns, 128):
        total += rows8[:, i : i + 128]
    return total


def reduced(p, total, mine, others, send_sems, recv_sems):
    at = 0
    for stage, devices in enumerate((p.near(), [p.along("x", k)[1] for k in range(1, p.side)])):
        sems = send_sems.at[stage], recv_sems.at[stage]
        mine[stage] = total
        for i, device in enumerate(devices):
            send(mine.at[stage], others.at[at + i], sems, device).start()
        came = others.at[pl.ds(at, len(devices))]
        send(came, came, sems, p.partner()).wait()
        for i in range(len(devices)):
            total = total + others[at + i]
        at += len(devices)
    return total


def rms(wide):
    return lax.rsqrt(jnp.mean(wide * wide, -1, keepdims=True) + 1e-6)


def kernel(side, count, x_in, dy_in, g_in, u_in, d_in, *refs):
    outs, (wg, wu, wd, a, a_t, b, b_t, h, acc, p3, squares, others), refs = refs[:3], refs[3:15], refs[15:]
    (gg, gu, gd, pg, pu, pd, sg, su, sd, lg, lu, ld, mg, mu, md, eg, eu, ed), refs = refs[:18], refs[18:]
    ag_send, ag_recv, rs_send, rs_recv, local, norm_send, norm_recv, free = refs
    p = Place(side)
    layers, tokens, depth = a.shape
    hidden = wg.shape[-1]
    chunks = hidden // CHUNK
    steps = layers * chunks
    flat_g, flat_u = (w.reshape(layers, depth, hidden) for w in (wg, wu))
    flat_d = wd.reshape(layers, hidden, depth)

    def shards():
        for i, (shard, whole) in enumerate(((g_in, wg), (u_in, wu), (d_in, wd))):
            for n in range(layers):
                yield pltpu.make_async_copy(shard.at[n], whole.at[n, p.x, p.y, p.c], local.at[i * layers + n])

    def load(i):
        source, target = ((x_in, h), (dy_in, b))[i]
        return pltpu.make_async_copy(source.at[0], target, local.at[3 * layers + i])

    for copy in shards():
        copy.start()
    for i in range(2):
        load(i).start()

    pairs = []

    def pair(*units):
        made = []
        for whole, rows, cols, first in units:
            at = 2 * (len(pairs) % WINDOW) + len(made)
            made.append(Gather(p, whole, rows, cols, ag_send.at[at], ag_recv.at[at], first))
        pairs.append(made)

    def chunk_pair(n, j):
        rows, cols = pl.ds(0, g_in.shape[1]), pl.ds(j * CHUNK, CHUNK)
        pair((wg.at[n], rows, cols, "x"), (wu.at[n], rows, cols, "y"))

    def down_pairs(n):
        rows, cols = d_in.shape[1] // 2, depth // 2
        for k in range(2):
            pair(
                (wd.at[n], pl.ds(0, rows), pl.ds(k * cols, cols), "x"),
                (wd.at[n], pl.ds(rows, rows), pl.ds(k * cols, cols), "y"),
            )

    for n in range(layers):
        if n == layers - 1:
            down_pairs(n)
        for j in range(chunks):
            if n < layers - 1 and j == chunks // 2:
                down_pairs(n)
            chunk_pair(n, j)

    begins = [0, 1, 1, 2, 2, *range(3, len(pairs) - 2)]
    ends = [begin + len(units[0].stages) for begin, units in zip(begins, pairs)]

    def gather_round(r):
        for begin, end, units in reversed(list(zip(begins, ends, pairs))):
            for unit in units:
                if begin < r <= end:
                    unit.wait(r - begin - 1)
                if begin <= r < end:
                    unit.start(r - begin)

    def columns(j, n=None):
        if n is None:
            return pl.ds(pl.multiple_of(j * CHUNK, CHUNK), CHUNK)
        return pl.ds(pl.multiple_of(j * CHUNK + n * WIDE, WIDE), WIDE)

    def tiles(size, body):
        @pl.loop(0, tokens // size, unroll=2)
        def _(t):
            body(pl.ds(pl.multiple_of(t * size, size), size))

    bands = [pl.ds(i, TALL) for i in range(0, tokens, TALL)]

    def forward(n, j, slot):
        for i in range(BLOCKS):
            for rows in bands:
                gate, up = dot(a[n, rows, :], flat_g[n, :, columns(j, i)]), dot(a[n, rows, :], flat_u[n, :, columns(j, i)])
                p3[slot, rows, columns(0, i)] = (jax.nn.silu(gate) * up).astype(BF16)

    def down(n, parts, more):
        for i in range(depth // WIDE):
            cols = columns(0, i)
            for rows in bands:
                y = sum(dot(p3[slot, rows, :], flat_d[n, pl.ds(j * CHUNK, CHUNK), cols]) for j, slot in parts)
                if more:
                    acc[rows, cols] = y
                else:
                    y = (acc[rows, cols] + y).astype(BF16)
                    h[rows, cols] = h[rows, cols] + y

    def norms(n):
        def body(rows):
            wide = h[rows, :].astype(F32)
            scaled = (wide * rms(wide)).astype(BF16)
            a[n, rows, :] = scaled
            a_t[n, :, rows] = scaled.T

        tiles(ROWS, body)

    def transpose_b(rows):
        b_t[:, rows] = b[rows, :].T

    def backward(n, j):
        for i in range(BLOCKS):
            for rows in bands:
                gate, up = dot(a[n, rows, :], flat_g[n, :, columns(j, i)]), dot(a[n, rows, :], flat_u[n, :, columns(j, i)])
                by_z = dot_t(b[rows, :], flat_d[n, columns(j, i), :]).astype(BF16).astype(F32)
                s = jax.nn.sigmoid(gate)
                silu = gate * s
                cols = columns(0, i)
                p3[0, rows, cols] = (silu * up).astype(BF16)
                p3[1, rows, cols] = (by_z * up * (s + silu * (1 - s))).astype(BF16)
                p3[2, rows, cols] = (by_z * silu).astype(BF16)

    def by_normed(n, j):
        for i in range(depth // WIDE):
            cols = columns(0, i)
            for rows in bands:
                by_gate, by_up = dot_t(p3[1, rows, :], flat_g[n, cols, columns(j)]), dot_t(p3[2, rows, :], flat_u[n, cols, columns(j)])
                acc[rows, cols] += by_gate + by_up

    def by_states(rows):
        wide = h[rows, :].astype(F32)
        scale = rms(wide)
        by = acc[rows, :].astype(BF16).astype(F32)
        along = jnp.sum(by * wide, -1, keepdims=True) * (scale * scale * scale) * (1 / depth)
        new = b[rows, :] + (by * scale - wide * along).astype(BF16)
        b[rows, :] = new
        b_t[:, rows] = new.T

    flat_gg, flat_gu = (r.reshape(CORES, depth, CHUNK) for r in (gg, gu))
    flat_gd = gd.reshape(CORES, CHUNK, depth)

    def scatters(q):
        slot, j = lax.rem(q, 2), lax.rem(q, chunks)
        sems = [(rs_send.at[slot, i], rs_recv.at[slot, i]) for i in range(3)]
        at = lambda *refs: [r.at[slot] for r in refs]
        g = Scatter(p, (*at(gg, pg), sg, *at(lg), mg, *at(eg)), *sems[0], "x")
        u = Scatter(p, (*at(gu, pu), su, *at(lu), mu, *at(eu)), *sems[1], "y")
        d = ScatterRows(p, (*at(gd, pd), sd, *at(ld), md, *at(ed)), *sems[2], j)
        return g, u, d

    def finish(q):
        n, j = layers - 1 - q // chunks, lax.rem(q, chunks)
        g, u, d = scatters(q)

        def keep(out, *where):
            def write(total):
                wide = total.astype(F32)
                out[where] = wide
                squares[2] = squares[2] + fold(wide * wide)

            return write

        og, ou, od = outs
        for unit, write in ((g, keep(og, n, slice(None), columns(j))), (u, keep(ou, n, slice(None), columns(j))), (d, keep(od, n))):
            unit.wait(2)
            unit.result(write)

        @pl.when(q + 2 < steps)
        def _():
            for other in p.others():
                pl.semaphore_signal(free.at[lax.rem(q, 2)], inc=1, device_id=other, device_id_type=MESH)

    p.barrier()
    for copy in shards():
        copy.wait()
    starts = ends[len(pairs) - chunks]
    half = chunks // 2

    def last_down():
        down(0, [(j, j - half + 1) for j in range(half, chunks)], False)
        norms(1)
        acc[...] = jnp.zeros_like(acc)

    queue = [(j, functools.partial(forward, 0, j, j)) for j in range(half)]
    queue += [(half + 1, functools.partial(down, 0, [(j, j) for j in range(half)], True))]
    queue += [(j + 2, functools.partial(forward, 0, j, j - half + 1)) for j in range(half, chunks)]
    queue += [(chunks + 1, last_down)]
    work, at = {}, -1
    for needs, piece in queue:
        at = max(at + 1, ends[needs])
        work[at] = piece
    starts = max(starts, at)
    for r in range(starts + 1):
        gather_round(r)
        if r == 0:
            load(0).wait()
            norms(0)
        elif r == 1:
            load(1).wait()
            tiles(ROWS, transpose_b)
            squares[2] = jnp.zeros_like(squares[2])
        if r in work:
            work[r]()

    def by_weights(n, slot):
        by_gate, by_up = dot(a_t[n], p3[1]), dot(a_t[n], p3[2])
        flat_gg[slot] = by_gate.astype(BF16)
        flat_gu[slot] = by_up.astype(BF16)

    def by_down(slot):
        flat_gd[slot] = dot(b_t[...], p3[0]).astype(BF16).T

    def advance(units, stage):
        for unit in units:
            unit.wait(stage)
            unit.add(stage)
            unit.start(stage + 1)

    def rs0(q):
        advance(scatters(q)[:2], 0)

    def rs1(q):
        g, u, d = scatters(q)
        advance((g, u), 1)

    def rs3(q):
        advance(scatters(q)[2:], 1)

    def rs2(q):
        advance(scatters(q)[2:], 0)

    def transition():
        tiles(ROWS, by_states)

    @pl.loop(0, steps + 2)
    def _(q):
        n, j, slot = layers - 1 - q // chunks, lax.rem(q, chunks), lax.rem(q, 2)
        computes = q < steps
        follows = (q > 0) & (q <= steps)

        @pl.when(q == chunks)
        def _():
            transition()

        @pl.when(computes)
        def _():
            backward(n, j)

        @pl.when(follows)
        def _():
            rs0(q - 1)

        @pl.when(q >= 2)
        def _():
            finish(q - 2)

        @pl.when(computes & (q < chunks))
        def _():
            by_normed(n, j)

        for k in range(ends[-1] - starts):

            @pl.when(q == k)
            def _():
                gather_round(starts + 1 + k)

        @pl.when(computes)
        def _():
            by_down(slot)

            @pl.when(q >= 2)
            def _():
                pl.semaphore_wait(free.at[slot], len(p.others()))

            scatters(q)[2].start(0)

        @pl.when(follows)
        def _():
            rs3(q - 1)

        @pl.when(computes)
        def _():
            by_weights(n, slot)
            for unit in scatters(q)[:2]:
                unit.start(0)
            rs2(q)

        @pl.when(follows)
        def _():
            rs1(q - 1)

    total = jnp.sum(reduced(p, squares[2], squares, others, norm_send, norm_recv), keepdims=True)
    factor = jnp.minimum(1.0, 0.5 * lax.rsqrt(total / count + 1e-30))
    for out in outs:
        out[...] = out[...] * factor.reshape(1, 1, 1)


def gradients_of(side, x, dy, weights):
    w_gate, _, w_down = weights
    layers, rows, hidden = w_gate.shape
    rows_d, depth = w_down.shape[1:]
    tokens = x.shape[1]
    chunk, block, rest = (rows, CHUNK), (rows_d, depth), side - 1

    def whole(w):
        return pltpu.VMEM((layers, side, side, CORES) + w.shape[1:], BF16)

    def buffers(lead, lead_d):
        return [pltpu.VMEM(lead + chunk, BF16)] * 2 + [pltpu.VMEM(lead_d + block, BF16)]

    sums = 3 * side - 2
    count = side * side * CORES * sum(w.size for w in weights)
    return pl.pallas_call(
        functools.partial(kernel, side, count),
        out_shape=[jax.ShapeDtypeStruct(w.shape, F32) for w in weights],
        in_specs=[HBM] * 5,
        out_specs=[VMEM] * 3,
        scratch_shapes=[whole(w) for w in weights]
        + [
            pltpu.VMEM((layers, tokens, depth), BF16),
            pltpu.VMEM((layers, depth, tokens), BF16),
            pltpu.VMEM((tokens, depth), BF16),
            pltpu.VMEM((depth, tokens), BF16),
            pltpu.VMEM((tokens, depth), BF16),
            pltpu.VMEM((tokens, depth), F32),
            pltpu.VMEM((3, tokens, CHUNK), BF16),
            pltpu.VMEM((3, 8, 128), F32),
            pltpu.VMEM((sums, 8, 128), F32),
        ]

        + buffers((2, side, side, CORES), (2, side, CORES))
        + buffers((2, side, side), (2, side))
        + buffers((side, side), (side,))
        + buffers((2, rest, side), (2, rest))
        + buffers((side,), ())
        + buffers((2, rest), (2, rest))
        + [
            pltpu.SemaphoreType.DMA((2 * WINDOW, GATHER_STEPS)),
            pltpu.SemaphoreType.DMA((2 * WINDOW, GATHER_STEPS)),
            pltpu.SemaphoreType.DMA((2, 3, SCATTER_STEPS)),
            pltpu.SemaphoreType.DMA((2, 3, SCATTER_STEPS)),
            pltpu.SemaphoreType.DMA((3 * layers + 2,)),
            pltpu.SemaphoreType.DMA((2,)),
            pltpu.SemaphoreType.DMA((2,)),
            pltpu.SemaphoreType.REGULAR((2,)),
        ],
        compiler_params=pltpu.CompilerParams(collective_id=0, has_side_effects=True, vmem_limit_bytes=67043328),
        name="gradients",
    )(x, dy, *weights)


def solution(mesh):
    side = math.isqrt(mesh.shape["dp"] // CORES)

    def step(x, dy, *arrays):
        weights, m, v = (arrays[i : i + 3] for i in (0, 3, 6))
        gradients = gradients_of(side, x, dy, weights)
        new = [adamw(w.astype(F32), m, v, g) for w, m, v, g in zip(weights, m, v, gradients, strict=True)]
        return tuple(one[which] for which in range(3) for one in new)

    states, cut = P(("rep", "dp"), None, None), P(None, "dp", None)
    return jax.shard_map(
        step,
        mesh=mesh,
        in_specs=(states, states) + (cut,) * 9,
        out_specs=(P("rep", "dp", None),) * 9,
        check_vma=False,
    )
```

```python
import functools
import math

import jax
import jax.numpy as jnp
from jax import lax
from jax.experimental import pallas as pl
from jax.experimental.pallas import tpu as pltpu
from jax.sharding import PartitionSpec as P

MESH = pl.DeviceIdType.MESH
CORES = 2
WIDE = 256
BLOCKS = 3
CHUNK = WIDE * BLOCKS
GATHER_STEPS = 5
SCATTER_STEPS = 3
TALL = 512
ROWS = 256
EARLY = 2
WINDOW = 8
VMEM = pl.BlockSpec(memory_space=pltpu.VMEM)
HBM = pl.BlockSpec(memory_space=pl.ANY)
BF16, F32 = jnp.bfloat16, jnp.float32


def dot(a, b):
    return jnp.dot(a, b, preferred_element_type=F32)


def dot_t(a, b):
    return lax.dot_general(a, b, (((1,), (1,)), ((), ())), preferred_element_type=F32)


def adamw(w, m, v, g):
    m = 0.9 * m + 0.1 * g
    v = 0.95 * v + 0.05 * g * g
    step = m * lax.rsqrt(v + 1e-8) + 0.1 * w
    return (w - 0.02 * step).astype(BF16), m, v


class Place:
    def __init__(self, side):
        self.side = side
        me = lax.axis_index("dp")
        self.c = lax.rem(me, CORES)
        self.y = lax.rem(me // CORES, side)
        self.x = me // (CORES * side)

    def device(self, x, y, c):
        return {"dp": (x * self.side + y) * CORES + c}

    def partner(self):
        return self.device(self.x, self.y, 1 - self.c)

    def along(self, axis, k):
        if axis == "x":
            x = lax.rem(self.x + k + self.side, self.side)
            return x, self.device(x, self.y, self.c)
        y = lax.rem(self.y + k + self.side, self.side)
        return y, self.device(self.x, y, self.c)

    def others(self):
        return [self.partner()] + [self.along(a, k)[1] for a in "xy" for k in range(1, self.side)]

    def near(self):
        ys = [self.along("y", k)[0] for k in range(self.side)]
        return [self.partner()] + [self.device(self.x, y, c) for y in ys[1:] for c in (self.c, 1 - self.c)]

    def barrier(self):
        sem = pltpu.get_barrier_semaphore()
        greeted = self.near() + [self.along("x", k)[1] for k in range(1, self.side)]
        for other in greeted:
            pl.semaphore_signal(sem, inc=1, device_id=other, device_id_type=MESH)
        pl.semaphore_wait(sem, len(greeted))


def send(src, dst, sems, device):
    return pltpu.make_async_remote_copy(
        src_ref=src, dst_ref=dst, send_sem=sems[0], recv_sem=sems[1], device_id=device, device_id_type=MESH
    )


class Gather:
    def __init__(self, place, whole, rows, cols, send_sems, recv_sems, first):
        p = place
        sems = [(send_sems.at[i], recv_sems.at[i]) for i in range(GATHER_STEPS)]
        second = "y" if first == "x" else "x"
        half = cols.size // 2
        halves = [pl.ds(cols.start, half), pl.ds(cols.start + half, half)]

        def block(i, cols):
            return whole.at[i, p.y, p.c, rows, cols] if first == "x" else whole.at[p.x, i, p.c, rows, cols]

        def line(i, cols):
            return whole.at[:, i, p.c, rows, cols] if first == "x" else whole.at[i, :, p.c, rows, cols]

        self.stages = []
        both = pl.ds(0, 2)
        for axis, part in ((first, block), (second, line)):
            me = p.along(axis, 0)[0]
            (after, up), (before, down) = p.along(axis, 1), p.along(axis, -1)
            mine = part(me, cols)
            self.stages.append(([(mine, up), (mine, down)], part(both, cols)))
            self.stages.append(([(part(before, halves[0]), up), (part(after, halves[1]), down)], part(both, halves[0])))
        plane = whole.at[:, :, p.c, rows, cols]
        self.stages.append(([(plane, p.partner())], plane))
        self.sems, self.partner = sems, p.partner()

    def start(self, stage):
        for part, device in self.stages[stage][0]:
            send(part, part, self.sems[stage], device).start()

    def wait(self, stage):
        total = self.stages[stage][1]
        send(total, total, self.sems[stage], self.partner).wait()


class Scatter:
    def __init__(self, place, refs, send_sems, recv_sems, first):
        p, s = place, place.side
        self.p, self.s, self.first, self.refs = p, s, first, refs
        mine, pair, paired, line, lined, last = refs
        self.sems = [(send_sems.at[i], recv_sems.at[i]) for i in range(SCATTER_STEPS)]
        second = "y" if first == "x" else "x"
        self.totals = pair, line, last
        self.stages = [[(mine.at[:, :, 1 - p.c], pair, p.partner())], [], []]
        for k in range(1, s):
            there, device = p.along(first, k)
            part = paired.at[there] if first == "x" else paired.at[:, there]
            self.stages[1].append((part, line.at[k - 1], device))
        for k in range(1, s):
            there, device = p.along(second, k)
            self.stages[2].append((lined.at[there], last.at[k - 1], device))

    def start(self, stage):
        for src, dst, device in self.stages[stage]:
            send(src, dst, self.sems[stage], device).start()

    def wait(self, stage):
        total = self.totals[stage]
        send(total, total, self.sems[stage], self.p.partner()).wait()

    def _pair_sum(self, x, y):
        mine, pair = self.refs[:2]
        return mine[x, y, self.p.c].astype(F32) + pair[x, y].astype(F32)

    def _line_sum(self, i):
        p, line = self.p, self.refs[3]
        total = self._pair_sum(p.x, i) if self.first == "x" else self._pair_sum(i, p.y)
        for k in range(self.s - 1):
            total += line[k, i].astype(F32)
        return total

    def add(self, stage):
        s = self.s
        _, _, paired, _, lined, _ = self.refs
        if stage == 0:

            @pl.loop(0, s * s, unroll=4)
            def _(i):
                x, y = i // s, lax.rem(i, s)
                paired[x, y] = self._pair_sum(x, y).astype(BF16)

        else:

            @pl.loop(0, s, unroll=True)
            def _(i):
                lined[i] = self._line_sum(i).astype(BF16)

    def result(self, write):
        p, last = self.p, self.refs[5]
        total = self._line_sum(p.y if self.first == "x" else p.x)
        for k in range(self.s - 1):
            total += last[k].astype(F32)
        write(total.astype(BF16))


class ScatterRows:
    def __init__(self, place, refs, send_sems, recv_sems, owner):
        p, s = place, place.side
        self.p, self.s, self.refs, self.owner = p, s, refs, owner
        mine, pair, paired, line, lined, last = refs
        self.sems = [(send_sems.at[i], recv_sems.at[i]) for i in range(SCATTER_STEPS)]
        self.totals = pair, line, last
        self.first = [(mine.at[:, 1 - p.c], pair, p.partner())]
        self.second = []
        for k in range(1, s):
            there, device = p.along("y", k)
            self.second.append((paired.at[there], line.at[k - 1], device))
        self.away = lax.rem(owner - p.x + s, s)

    def _last(self, k):
        lined, last = self.refs[4:]
        return send(lined, last.at[k - 1], self.sems[2], self.p.device(self.owner, self.p.y, self.p.c))

    def start(self, stage):
        if stage < 2:
            for src, dst, device in (self.first, self.second)[stage]:
                send(src, dst, self.sems[stage], device).start()
        else:
            for k in range(1, self.s):

                @pl.when(self.away == k)
                def _():
                    self._last(k).start()

    def wait(self, stage):
        total = self.totals[stage]
        whole = lambda: send(total, total, self.sems[stage], self.p.partner())
        if stage < 2:
            whole().wait()
        else:

            @pl.when(self.away > 0)
            def _():
                self._last(1).wait_send()

            @pl.when(self.away == 0)
            def _():
                whole().wait_recv()

    def _pair_sum(self, y):
        mine, pair = self.refs[:2]
        return mine[y, self.p.c].astype(F32) + pair[y].astype(F32)

    def _line_sum(self):
        total = self._pair_sum(self.p.y)
        for k in range(self.s - 1):
            total += self.refs[3][k].astype(F32)
        return total

    def add(self, stage):
        _, _, paired, _, lined, _ = self.refs
        if stage == 0:

            @pl.loop(0, self.s, unroll=True)
            def _(y):
                paired[y] = self._pair_sum(y).astype(BF16)

        else:
            lined[...] = self._line_sum().astype(BF16)

    def result(self, write):
        @pl.when(self.away == 0)
        def _():
            total = self._line_sum()
            for k in range(self.s - 1):
                total += self.refs[5][k].astype(F32)
            write(total.astype(BF16))


def fold(wide):
    rows, columns = wide.shape
    rows8 = wide.reshape(rows // 8, 8, columns).sum(0)
    total = rows8[:, :128]
    for i in range(128, columns, 128):
        total += rows8[:, i : i + 128]
    return total


def reduced(p, total, mine, others, send_sems, recv_sems):
    at = 0
    for stage, devices in enumerate((p.near(), [p.along("x", k)[1] for k in range(1, p.side)])):
        sems = send_sems.at[stage], recv_sems.at[stage]
        mine[stage] = total
        for i, device in enumerate(devices):
            send(mine.at[stage], others.at[at + i], sems, device).start()
        came = others.at[pl.ds(at, len(devices))]
        send(came, came, sems, p.partner()).wait()
        for i in range(len(devices)):
            total = total + others[at + i]
        at += len(devices)
    return total


def rms(wide):
    return lax.rsqrt(jnp.mean(wide * wide, -1, keepdims=True) + 1e-6)


def kernel(side, count, x_in, dy_in, g_in, u_in, d_in, *refs):
    outs, (wg, wu, wd, a, a_t, b, b_t, h, acc, p3, squares, others), refs = refs[:3], refs[3:15], refs[15:]
    (gg, gu, gd, pg, pu, pd, sg, su, sd, lg, lu, ld, mg, mu, md, eg, eu, ed), refs = refs[:18], refs[18:]
    ag_send, ag_recv, rs_send, rs_recv, local, norm_send, norm_recv, free = refs
    p = Place(side)
    layers, tokens, depth = a.shape
    hidden = wg.shape[-1]
    chunks = hidden // CHUNK
    steps = layers * chunks
    flat_g, flat_u = (w.reshape(layers, depth, hidden) for w in (wg, wu))
    flat_d = wd.reshape(layers, hidden, depth)

    def shards():
        for i, (shard, whole) in enumerate(((g_in, wg), (u_in, wu), (d_in, wd))):
            for n in range(layers):
                yield pltpu.make_async_copy(shard.at[n], whole.at[n, p.x, p.y, p.c], local.at[i * layers + n])

    def load(i):
        source, target = ((x_in, h), (dy_in, b))[i]
        return pltpu.make_async_copy(source.at[0], target, local.at[3 * layers + i])

    for copy in shards():
        copy.start()
    for i in range(2):
        load(i).start()

    pairs = []

    def pair(*units):
        made = []
        for whole, rows, cols, first in units:
            at = 2 * (len(pairs) % WINDOW) + len(made)
            made.append(Gather(p, whole, rows, cols, ag_send.at[at], ag_recv.at[at], first))
        pairs.append(made)

    def chunk_pair(n, j):
        rows, cols = pl.ds(0, g_in.shape[1]), pl.ds(j * CHUNK, CHUNK)
        pair((wg.at[n], rows, cols, "x"), (wu.at[n], rows, cols, "y"))

    def down_pairs(n):
        rows, cols = d_in.shape[1] // 2, depth // 2
        for k in range(2):
            pair(
                (wd.at[n], pl.ds(0, rows), pl.ds(k * cols, cols), "x"),
                (wd.at[n], pl.ds(rows, rows), pl.ds(k * cols, cols), "y"),
            )

    for n in range(layers):
        if n == layers - 1:
            down_pairs(n)
        for j in range(chunks):
            if n < layers - 1 and j == chunks // 2:
                down_pairs(n)
            chunk_pair(n, j)

    begins = [0, 1, 1, 2, 2, 3, 3, *range(4, len(pairs) - 3)]
    ends = [begin + len(units[0].stages) for begin, units in zip(begins, pairs)]

    def gather_round(r):
        for begin, end, units in reversed(list(zip(begins, ends, pairs))):
            for unit in units:
                if begin < r <= end:
                    unit.wait(r - begin - 1)
                if begin <= r < end:
                    unit.start(r - begin)

    def columns(j, n=None):
        if n is None:
            return pl.ds(pl.multiple_of(j * CHUNK, CHUNK), CHUNK)
        return pl.ds(pl.multiple_of(j * CHUNK + n * WIDE, WIDE), WIDE)

    def tiles(size, body):
        @pl.loop(0, tokens // size, unroll=2)
        def _(t):
            body(pl.ds(pl.multiple_of(t * size, size), size))

    bands = [pl.ds(i, TALL) for i in range(0, tokens, TALL)]

    def forward(n, j, slot):
        for i in range(BLOCKS):
            for rows in bands:
                gate, up = dot(a[n, rows, :], flat_g[n, :, columns(j, i)]), dot(a[n, rows, :], flat_u[n, :, columns(j, i)])
                p3[slot, rows, columns(0, i)] = (jax.nn.silu(gate) * up).astype(BF16)

    def down(n, parts, more):
        for i in range(depth // WIDE):
            cols = columns(0, i)
            for rows in bands:
                y = sum(dot(p3[slot, rows, :], flat_d[n, pl.ds(j * CHUNK, CHUNK), cols]) for j, slot in parts)
                if more:
                    acc[rows, cols] = y
                else:
                    y = (acc[rows, cols] + y).astype(BF16)
                    h[rows, cols] = h[rows, cols] + y

    def norms(n):
        def body(rows):
            wide = h[rows, :].astype(F32)
            scaled = (wide * rms(wide)).astype(BF16)
            a[n, rows, :] = scaled
            a_t[n, :, rows] = scaled.T

        tiles(ROWS, body)

    def transpose_b(rows):
        b_t[:, rows] = b[rows, :].T

    def backward(n, j):
        for i in range(BLOCKS):
            for rows in bands:
                gate, up = dot(a[n, rows, :], flat_g[n, :, columns(j, i)]), dot(a[n, rows, :], flat_u[n, :, columns(j, i)])
                by_z = dot_t(b[rows, :], flat_d[n, columns(j, i), :]).astype(BF16).astype(F32)
                s = jax.nn.sigmoid(gate)
                silu = gate * s
                cols = columns(0, i)
                p3[0, rows, cols] = (silu * up).astype(BF16)
                p3[1, rows, cols] = (by_z * up * (s + silu * (1 - s))).astype(BF16)
                p3[2, rows, cols] = (by_z * silu).astype(BF16)

    def by_normed(n, j):
        for i in range(depth // WIDE):
            cols = columns(0, i)
            for rows in bands:
                by_gate, by_up = dot_t(p3[1, rows, :], flat_g[n, cols, columns(j)]), dot_t(p3[2, rows, :], flat_u[n, cols, columns(j)])
                acc[rows, cols] += by_gate + by_up

    def by_states(rows):
        wide = h[rows, :].astype(F32)
        scale = rms(wide)
        by = acc[rows, :].astype(BF16).astype(F32)
        along = jnp.sum(by * wide, -1, keepdims=True) * (scale * scale * scale) * (1 / depth)
        new = b[rows, :] + (by * scale - wide * along).astype(BF16)
        b[rows, :] = new
        b_t[:, rows] = new.T

    flat_gg, flat_gu = (r.reshape(CORES, depth, CHUNK) for r in (gg, gu))
    flat_gd = gd.reshape(CORES, CHUNK, depth)

    def scatters(q):
        slot, j = lax.rem(q, 2), lax.rem(q, chunks)
        sems = [(rs_send.at[slot, i], rs_recv.at[slot, i]) for i in range(3)]
        at = lambda *refs: [r.at[slot] for r in refs]
        g = Scatter(p, (*at(gg, pg), sg, *at(lg), mg, *at(eg)), *sems[0], "x")
        u = Scatter(p, (*at(gu, pu), su, *at(lu), mu, *at(eu)), *sems[1], "y")
        d = ScatterRows(p, (*at(gd, pd), sd, *at(ld), md, *at(ed)), *sems[2], j)
        return g, u, d

    def finish(q):
        n, j = layers - 1 - q // chunks, lax.rem(q, chunks)
        g, u, d = scatters(q)

        def keep(out, *where):
            def write(total):
                wide = total.astype(F32)
                out[where] = wide
                squares[2] = squares[2] + fold(wide * wide)

            return write

        og, ou, od = outs
        for unit, write in ((g, keep(og, n, slice(None), columns(j))), (u, keep(ou, n, slice(None), columns(j))), (d, keep(od, n))):
            unit.wait(2)
            unit.result(write)

        @pl.when(q + 2 < steps)
        def _():
            for other in p.others():
                pl.semaphore_signal(free.at[lax.rem(q, 2)], inc=1, device_id=other, device_id_type=MESH)

    p.barrier()
    for copy in shards():
        copy.wait()
    starts = ends[len(pairs) - chunks]
    half = chunks // 2

    def last_down():
        down(0, [(j, j - half + 1) for j in range(half, chunks)], False)
        norms(1)
        acc[...] = jnp.zeros_like(acc)

    queue = [(j, functools.partial(forward, 0, j, j)) for j in range(half)]
    queue += [(half + 1, functools.partial(down, 0, [(j, j) for j in range(half)], True))]
    queue += [(j + 2, functools.partial(forward, 0, j, j - half + 1)) for j in range(half, chunks)]
    queue += [(chunks + 1, last_down)]
    work, at = {}, -1
    for needs, piece in queue:
        at = max(at + 1, ends[needs])
        work[at] = piece
    starts = max(starts, at)
    for r in range(starts + 1):
        gather_round(r)
        if r == 0:
            load(0).wait()
            norms(0)
        elif r == 1:
            load(1).wait()
            tiles(ROWS, transpose_b)
            squares[2] = jnp.zeros_like(squares[2])
        if r in work:
            work[r]()

    def by_weights(n, slot):
        by_gate, by_up = dot(a_t[n], p3[1]), dot(a_t[n], p3[2])
        flat_gg[slot] = by_gate.astype(BF16)
        flat_gu[slot] = by_up.astype(BF16)

    def by_down(slot):
        flat_gd[slot] = dot(b_t[...], p3[0]).astype(BF16).T

    def advance(units, stage):
        for unit in units:
            unit.wait(stage)
            unit.add(stage)
            unit.start(stage + 1)

    def rs0(q):
        advance(scatters(q)[:2], 0)

    def rs1(q):
        g, u, d = scatters(q)
        advance((g, u), 1)

    def rs3(q):
        advance(scatters(q)[2:], 1)

    def rs2(q):
        advance(scatters(q)[2:], 0)

    def transition():
        tiles(ROWS, by_states)

    @pl.loop(0, steps + 2)
    def _(q):
        n, j, slot = layers - 1 - q // chunks, lax.rem(q, chunks), lax.rem(q, 2)
        computes = q < steps
        follows = (q > 0) & (q <= steps)

        @pl.when(q == chunks)
        def _():
            transition()

        @pl.when(computes)
        def _():
            backward(n, j)

        @pl.when(follows)
        def _():
            rs0(q - 1)

        @pl.when(q >= 2)
        def _():
            finish(q - 2)

        @pl.when(computes & (q < chunks))
        def _():
            by_normed(n, j)

        for k in range(ends[-1] - starts):

            @pl.when(q == k)
            def _():
                gather_round(starts + 1 + k)

        @pl.when(computes)
        def _():
            by_down(slot)

            @pl.when(q >= 2)
            def _():
                pl.semaphore_wait(free.at[slot], len(p.others()))

            scatters(q)[2].start(0)

        @pl.when(follows)
        def _():
            rs3(q - 1)

        @pl.when(computes)
        def _():
            by_weights(n, slot)
            for unit in scatters(q)[:2]:
                unit.start(0)
            rs2(q)

        @pl.when(follows)
        def _():
            rs1(q - 1)

    total = jnp.sum(reduced(p, squares[2], squares, others, norm_send, norm_recv), keepdims=True)
    factor = jnp.minimum(1.0, 0.5 * lax.rsqrt(total / count + 1e-30))
    for out in outs:
        out[...] = out[...] * factor.reshape(1, 1, 1)


def gradients_of(side, x, dy, weights):
    w_gate, _, w_down = weights
    layers, rows, hidden = w_gate.shape
    rows_d, depth = w_down.shape[1:]
    tokens = x.shape[1]
    chunk, block, rest = (rows, CHUNK), (rows_d, depth), side - 1

    def whole(w):
        return pltpu.VMEM((layers, side, side, CORES) + w.shape[1:], BF16)

    def buffers(lead, lead_d):
        return [pltpu.VMEM(lead + chunk, BF16)] * 2 + [pltpu.VMEM(lead_d + block, BF16)]

    sums = 3 * side - 2
    count = side * side * CORES * sum(w.size for w in weights)
    return pl.pallas_call(
        functools.partial(kernel, side, count),
        out_shape=[jax.ShapeDtypeStruct(w.shape, F32) for w in weights],
        in_specs=[HBM] * 5,
        out_specs=[VMEM] * 3,
        scratch_shapes=[whole(w) for w in weights]
        + [
            pltpu.VMEM((layers, tokens, depth), BF16),
            pltpu.VMEM((layers, depth, tokens), BF16),
            pltpu.VMEM((tokens, depth), BF16),
            pltpu.VMEM((depth, tokens), BF16),
            pltpu.VMEM((tokens, depth), BF16),
            pltpu.VMEM((tokens, depth), F32),
            pltpu.VMEM((3, tokens, CHUNK), BF16),
            pltpu.VMEM((3, 8, 128), F32),
            pltpu.VMEM((sums, 8, 128), F32),
        ]

        + buffers((2, side, side, CORES), (2, side, CORES))
        + buffers((2, side, side), (2, side))
        + buffers((side, side), (side,))
        + buffers((2, rest, side), (2, rest))
        + buffers((side,), ())
        + buffers((2, rest), (2, rest))
        + [
            pltpu.SemaphoreType.DMA((2 * WINDOW, GATHER_STEPS)),
            pltpu.SemaphoreType.DMA((2 * WINDOW, GATHER_STEPS)),
            pltpu.SemaphoreType.DMA((2, 3, SCATTER_STEPS)),
            pltpu.SemaphoreType.DMA((2, 3, SCATTER_STEPS)),
            pltpu.SemaphoreType.DMA((3 * layers + 2,)),
            pltpu.SemaphoreType.DMA((2,)),
            pltpu.SemaphoreType.DMA((2,)),
            pltpu.SemaphoreType.REGULAR((2,)),
        ],
        compiler_params=pltpu.CompilerParams(collective_id=0, has_side_effects=True, vmem_limit_bytes=67043328),
        name="gradients",
    )(x, dy, *weights)


def solution(mesh):
    side = math.isqrt(mesh.shape["dp"] // CORES)

    def step(x, dy, *arrays):
        weights, m, v = (arrays[i : i + 3] for i in (0, 3, 6))
        gradients = gradients_of(side, x, dy, weights)
        new = [adamw(w.astype(F32), m, v, g) for w, m, v, g in zip(weights, m, v, gradients, strict=True)]
        return tuple(one[which] for which in range(3) for one in new)

    states, cut = P(("rep", "dp"), None, None), P(None, "dp", None)
    return jax.shard_map(
        step,
        mesh=mesh,
        in_specs=(states, states) + (cut,) * 9,
        out_specs=(P("rep", "dp", None),) * 9,
        check_vma=False,
    )
```
